1024 devices in a mesh: face: 32 (over z_lo, y), col: 32 (over z_hi, x, core).
Axes of the slice: x: 4, y: 8, z: 16 (z_hi: 4, z_lo: 4; z = z_hi * 4 + z_lo), core: 2. Of those that a mesh axis runs over, the one named last changes fastest.
Arguments:
- fields: float32 [4, 640, 640, 128], P(None, 'face', 'col'), may hold values from -6 to 6
- metric_diag: float32 [2, 640, 640], P(None, 'face', 'col'), may hold values from 0.05 to 0.5
- metric_cross: float32 [640, 640], P('face', 'col'), may hold values from -0.1 to 0.1
- point_mass: float32 [640, 640], P('face', 'col'), may hold values from 0.5 to 2
Outputs:
- biharmonic: float32 [4, 640, 640, 128], P(None, 'face', 'col')
The draws below stay inside these ranges and needn't reach their ends.
All inputs are finite; a program needn't handle non-finite values.
Results may differ from the reference program's by a relative error of at most 0.00024.
Values sent between devices are 32-bit elements; how exact they have to be, the bound alone decides.
A program may use at most 32 MiB of HBM per device.

```python
import math
import jax
import jax.numpy as jnp
import numpy as np
from jax import lax

FIELDS = 4
LEV = 128
NXP = 640
NYP = 640


def block_levels(key, shape, split, low, top_value):
    loudness = 1.0
    for axis_at, blocks in split:
        steps = jax.random.uniform(jax.random.fold_in(jax.random.fold_in(key, 6), axis_at), (blocks,), jnp.float32, low / len(split), top_value / len(split))
        loudness = loudness * jnp.repeat(jnp.exp(steps), shape[axis_at] // blocks).reshape((-1,) + (1,) * (len(shape) - 1 - axis_at))
    return loudness


def noise(own_key, shape, scale, bound, pieces=(), held_as=jnp.bfloat16):
    factor_of = block_levels(own_key, shape, pieces, -0.22, 0.18) if pieces else 1.0
    result = jax.random.normal(own_key, shape, jnp.float32) * scale * factor_of
    return jnp.minimum(jnp.maximum(result, -bound), bound).astype(held_as)


def setup_inputs(seed: int = 0) -> dict:
    key_list = jax.random.split(jax.random.key(seed), 5)
    fields = noise(key_list[0], (FIELDS, NXP, NYP, LEV), 1.0, 6.0, ((1, 32), (2, 32)), jnp.float32)
    metric_diag = jnp.clip(jnp.exp(math.log(0.5) - 2.3025851 * jax.random.uniform(key_list[1], (2, NXP, NYP), jnp.float32) ** block_levels(key_list[1], (2, NXP, NYP), ((1, 32), (2, 32)), -0.2, 0.2)), 0.05, 0.5)
    metric_cross = jnp.clip(jax.random.uniform(key_list[2], (NXP, NYP), jnp.float32, -0.1, 0.1) * block_levels(key_list[2], (NXP, NYP), ((0, 32), (1, 32)), -0.4, 0.0), -0.1, 0.1)
    point_mass = jnp.clip(jnp.exp(math.log(2.0) - 1.3862944 * jax.random.uniform(key_list[3], (NXP, NYP), jnp.float32) ** block_levels(key_list[3], (NXP, NYP), ((0, 32), (1, 32)), -0.2, 0.2)), 0.5, 2.0)
    return dict(fields=fields, metric_diag=metric_diag, metric_cross=metric_cross, point_mass=point_mass)


def derivative_table():
    small = 1.0 / np.sqrt(5.0)
    nodes = np.array([-1.0, -small, small, 1.0])
    count = nodes.shape[0]
    weights = np.array([np.prod([nodes[a] - nodes[k] for k in range(count) if k != a]) for a in range(count)])
    table = np.zeros((count, count))
    for a in range(count):
        for b in range(count):
            if a == b:
                table[a, b] = np.sum([1.0 / (nodes[a] - nodes[k]) for k in range(count) if k != a])
            else:
                table[a, b] = weights[a] / weights[b] / (nodes[a] - nodes[b])
    return jnp.asarray(table, jnp.float32)

def laplace(values, metric_diag, metric_cross):
    table = derivative_table()
    nfield, rows, cols, nlev = values.shape
    blocks_x = rows // 4
    blocks_y = cols // 4
    shaped = values.reshape(nfield, blocks_x, 4, blocks_y, 4, nlev)
    first_diag = metric_diag[0].reshape(1, blocks_x, 4, blocks_y, 4, 1)
    second_diag = metric_diag[1].reshape(1, blocks_x, 4, blocks_y, 4, 1)
    cross_term = metric_cross.reshape(1, blocks_x, 4, blocks_y, 4, 1)
    high = lax.Precision.HIGHEST
    grad_x = jnp.einsum('ab,febgcl->feagcl', table, shaped, precision=high)
    grad_y = jnp.einsum('cd,febgdl->febgcl', table, shaped, precision=high)
    flux_x = first_diag * grad_x + cross_term * grad_y
    flux_y = cross_term * grad_x + second_diag * grad_y
    weak = jnp.einsum('ba,febgcl->feagcl', table, flux_x, precision=high)
    weak = weak + jnp.einsum('dc,febgdl->febgcl', table, flux_y, precision=high)
    return (-weak).reshape(nfield, rows, cols, nlev)

def assemble(padded):
    rows = padded.shape[1] - 2
    cols = padded.shape[2] - 2
    row_local = jnp.arange(rows, dtype=jnp.int32) % 4
    col_local = jnp.arange(cols, dtype=jnp.int32) % 4
    row_low = (row_local == 0).astype(jnp.float32).reshape(1, rows, 1, 1)
    row_high = (row_local == 3).astype(jnp.float32).reshape(1, rows, 1, 1)
    col_low = (col_local == 0).astype(jnp.float32).reshape(1, 1, cols, 1)
    col_high = (col_local == 3).astype(jnp.float32).reshape(1, 1, cols, 1)
    summed = padded[:, 1:-1] + row_low * padded[:, :-2] + row_high * padded[:, 2:]
    return summed[:, :, 1:-1] + col_low * summed[:, :, :-2] + col_high * summed[:, :, 2:]

def wrap_pad(values):
    return jnp.pad(values, ((0, 0), (1, 1), (1, 1), (0, 0)), mode='wrap')

def reference(fields, metric_diag, metric_cross, point_mass):
    mass_sum = assemble(wrap_pad(point_mass[None, :, :, None]))
    first = assemble(wrap_pad(laplace(fields, metric_diag, metric_cross))) / mass_sum
    return assemble(wrap_pad(laplace(first, metric_diag, metric_cross))) / mass_sum
```

```python
import functools

import jax
import jax.numpy as jnp
import numpy as np
from jax import lax
from jax.experimental import pallas as pl
from jax.experimental.pallas import tpu as pltpu
from jax.sharding import PartitionSpec as P

MESH = pl.DeviceIdType.MESH
SUB = 8
LANES = 128


def derivative_table():
    small = 1.0 / np.sqrt(5.0)
    nodes = np.array([-1.0, -small, small, 1.0])
    count = nodes.shape[0]
    weights = np.array(
        [np.prod([nodes[a] - nodes[k] for k in range(count) if k != a]) for a in range(count)]
    )
    table = np.zeros((count, count))
    for a in range(count):
        for b in range(count):
            if a == b:
                table[a, b] = np.sum([1.0 / (nodes[a] - nodes[k]) for k in range(count) if k != a])
            else:
                table[a, b] = weights[a] / weights[b] / (nodes[a] - nodes[b])
    table[np.abs(table) < 1e-12] = 0.0
    return table


def combine(table, parts):
    out = []
    for a in range(4):
        total = None
        for b in range(4):
            if table[a, b] == 0.0:
                continue
            term = np.float32(table[a, b]) * parts[b]
            total = term if total is None else total + term
        out.append(total)
    return out


def shift_coefficients(table):
    local = lax.broadcasted_iota(jnp.int32, (SUB, LANES), 0) % 4
    result = {}
    for s in range(-3, 4):
        value = jnp.zeros((SUB, LANES), jnp.float32)
        for c in range(4):
            if 0 <= c + s < 4:
                value = jnp.where(local == c, np.float32(table[c, c + s]), value)
        result[s] = value
    return result


def along(tile, coefficients):
    total = coefficients[0] * tile
    for s in (-3, -2, -1, 1, 2, 3):
        total = total + coefficients[s] * pltpu.roll(tile, (-s) % SUB, 0)
    return total


def operator_kernel(
    faces, cols_axis, nfield, rows, cols,
    fields, diag, cross, mass,
    out,
    u, md, mc, mp, mpad, mrow, mside, mcorner, weights,
    lap1, lap2, send_w, send_e, halo_w, halo_e, result,
    load_sem, store_sem, mass_send, mass_recv, edge_send, edge_recv,
):
    table = derivative_table()
    blocks = rows // 4
    tiles = -(-cols // SUB)
    wide = tiles * SUB
    face = lax.axis_index("face")
    col = lax.axis_index("col")
    up, down = lax.rem(face + faces - 1, faces), lax.rem(face + 1, faces)
    left, right = lax.rem(col + cols_axis - 1, cols_axis), lax.rem(col + 1, cols_axis)
    partners = (
        (up, col), (down, col), (face, left), (face, right),
        (up, left), (up, right), (down, left), (down, right),
    )

    barrier = pltpu.get_barrier_semaphore()
    for partner in partners:
        pl.semaphore_signal(barrier, inc=1, device_id=partner, device_id_type=MESH)

    small_loads = [
        pltpu.make_async_copy(source, target, load_sem.at[nfield + k])
        for k, (source, target) in enumerate(((diag, md), (cross, mc), (mass, mp)))
    ]
    field_loads = [
        pltpu.make_async_copy(fields.at[f], u.at[f], load_sem.at[f]) for f in range(nfield)
    ]
    for load in small_loads + field_loads:
        load.start()

    sub = lax.broadcasted_iota(jnp.int32, (SUB, LANES), 0)

    def spread(k, square):
        turned = jnp.transpose(square)
        for r in range(rows):
            weights[k, r] = jnp.broadcast_to(turned[:wide, r : r + 1], (wide, LANES))

    def padded(value):
        block = jnp.zeros((LANES, LANES), jnp.float32)
        return lax.pad(value, np.float32(0), ((0, LANES - rows, 0), (0, LANES - cols, 0)))

    for load in small_loads:
        load.wait()
    mpad[...] = padded(mp[...])[:wide]
    spread(0, padded(md[0]))
    spread(1, padded(md[1]))
    spread(2, padded(mc[...]))

    forward = shift_coefficients(table)
    backward = shift_coefficients(table.T)

    def laplace(values, e, v):
        window = pl.ds(v * SUB, SUB)
        grad_x = combine(table, values)
        grad_y = [along(x, forward) for x in values]
        flux_x, flux_y = [], []
        for a in range(4):
            first, second, mixed = (weights[k, 4 * e + a, window, :] for k in range(3))
            flux_x.append(first * grad_x[a] + mixed * grad_y[a])
            flux_y.append(mixed * grad_x[a] + second * grad_y[a])
        weak = combine(table.T, flux_x)
        return [weak[a] + along(flux_y[a], backward) for a in range(4)]

    def keep(phase, lap, f, e, v, weak):
        for a in range(4):
            r = 4 * e + a
            lap[f, r + 1, pl.ds(v * SUB, SUB), :] = weak[a]
            if v == 0:
                send_w[phase, f, r] = weak[a][0:1]
            if v == tiles - 1:
                last = (cols - 1) % SUB
                send_e[phase, f, r] = weak[a][last : last + 1]

    def edge_copies(phase, lap, f):
        west, east = send_w.at[phase, f], send_e.at[phase, f]
        to_west, to_east = halo_e.at[phase, f], halo_w.at[phase, f]
        pairs = (
            (lap.at[f, 1], lap.at[f, rows + 1]),
            (lap.at[f, rows], lap.at[f, 0]),
            (west, to_west.at[pl.ds(1, rows)]),
            (east, to_east.at[pl.ds(1, rows)]),
            (west.at[0], to_west.at[rows + 1]),
            (east.at[0], to_east.at[rows + 1]),
            (west.at[rows - 1], to_west.at[0]),
            (east.at[rows - 1], to_east.at[0]),
        )
        return [
            pltpu.make_async_remote_copy(
                src_ref=source,
                dst_ref=target,
                send_sem=edge_send.at[phase, k, f],
                recv_sem=edge_recv.at[phase, k, f],
                device_id=partners[k],
                device_id_type=MESH,
            )
            for k, (source, target) in enumerate(pairs)
        ]

    low, high = mpad.at[pl.ds(0, SUB)], mpad.at[pl.ds(wide - SUB, SUB)]
    mass_pairs = (
        (low, mrow.at[1]), (high, mrow.at[0]),
        (mpad, mside.at[1]), (mpad, mside.at[0]),
        (low, mcorner.at[3]), (low, mcorner.at[2]),
        (high, mcorner.at[1]), (high, mcorner.at[0]),
    )
    mass_copies = [
        pltpu.make_async_remote_copy(
            src_ref=source,
            dst_ref=target,
            send_sem=mass_send.at[k],
            recv_sem=mass_recv.at[k],
            device_id=partners[k],
            device_id_type=MESH,
        )
        for k, (source, target) in enumerate(mass_pairs)
    ]

    def first_pass(f, carry):
        pltpu.make_async_copy(fields.at[f], u.at[f], load_sem.at[f]).wait()
        for e in range(blocks):
            for v in range(tiles):
                count = min(SUB, cols - v * SUB)
                values = []
                for a in range(4):
                    value = u[f, 4 * e + a, pl.ds(v * SUB, count), :]
                    if count < SUB:
                        value = lax.pad(value, np.float32(0), ((0, SUB - count, 0), (0, 0, 0)))
                    values.append(value)
                keep(0, lap1, f, e, v, laplace(values, e, v))
        return carry

    lax.fori_loop(0, nfield, first_pass, 0)

    pl.semaphore_wait(barrier, 8)
    for copy in mass_copies:
        copy.start()

    def send_first(f, carry):
        for copy in edge_copies(0, lap1, f):
            copy.start()
        return carry

    lax.fori_loop(0, nfield, send_first, 0)

    for copy in mass_copies:
        copy.wait_recv()
    rid = lax.broadcasted_iota(jnp.int32, (wide, LANES), 0)
    cid = lax.broadcasted_iota(jnp.int32, (wide, LANES), 1)
    zero = jnp.zeros((wide, LANES), jnp.float32)

    def down_rows(centre, north, south):
        total = centre
        inner_low = (rid % 4 == 0) & (rid > 0)
        inner_high = (rid % 4 == 3) & (rid < rows - 1)
        total = total + jnp.where(inner_low, pltpu.roll(centre, 1, 0), zero)
        total = total + jnp.where(inner_high, pltpu.roll(centre, wide - 1, 0), zero)
        before = jnp.broadcast_to(north, (wide, LANES))
        after = jnp.broadcast_to(south, (wide, LANES))
        total = total + jnp.where(rid == 0, before, zero)
        return total + jnp.where(rid == rows - 1, after, zero)

    last = (rows - 1) % SUB
    own = down_rows(mpad[...], mrow[0, last : last + 1], mrow[1, 0:1])
    west = down_rows(mside[0], mcorner[0, last : last + 1], mcorner[2, 0:1])
    east = down_rows(mside[1], mcorner[1, last : last + 1], mcorner[3, 0:1])
    total = own
    total = total + jnp.where((cid % 4 == 0) & (cid > 0), pltpu.roll(own, 1, 1), zero)
    total = total + jnp.where((cid % 4 == 3) & (cid < cols - 1), pltpu.roll(own, LANES - 1, 1), zero)
    total = total + jnp.where(cid == 0, pltpu.roll(west, LANES - cols + 1, 1), zero)
    total = total + jnp.where(cid == cols - 1, pltpu.roll(east, cols - 1, 1), zero)
    valid = (rid < rows) & (cid < cols)
    inverse = jnp.where(valid, 1.0 / jnp.where(valid, total, 1.0), 0.0)
    spread(3, jnp.concatenate([inverse, jnp.zeros((LANES - wide, LANES), jnp.float32)], axis=0))

    def assembled(phase, lap, f, r):
        parts = [lap[f, r + 1, pl.ds(v * SUB, SUB), :] for v in range(tiles)]
        side_w, side_e = halo_w[phase, f, r + 1], halo_e[phase, f, r + 1]
        other = None
        if r % 4 == 0:
            other = r
        elif r % 4 == 3:
            other = r + 2
        if other is not None:
            parts = [parts[v] + lap[f, other, pl.ds(v * SUB, SUB), :] for v in range(tiles)]
            side_w = side_w + halo_w[phase, f, other]
            side_e = side_e + halo_e[phase, f, other]
        prev = [pltpu.roll(x, 1, 0) for x in parts]
        nxt = [pltpu.roll(x, SUB - 1, 0) for x in parts]
        end = (cols - 1) % SUB
        out_tiles = []
        for v in range(tiles):
            before = jnp.broadcast_to(side_w, (SUB, LANES)) if v == 0 else prev[v - 1]
            add = jnp.where(sub == 0, before, jnp.where(sub == 4, prev[v], 0.0))
            if v < tiles - 1:
                add = jnp.where(sub == 3, nxt[v], jnp.where(sub == 7, nxt[v + 1], add))
            else:
                after = jnp.broadcast_to(side_e, (SUB, LANES))
                if end == 7:
                    add = jnp.where(sub == 3, nxt[v], add)
                add = jnp.where(sub == end, after, add)
            out_tiles.append((parts[v] + add) * weights[3, r, pl.ds(v * SUB, SUB), :])
        return out_tiles

    def second_pass(f, carry):
        for copy in edge_copies(0, lap1, f):
            copy.wait_recv()
        for e in range(blocks):
            values = [assembled(0, lap1, f, 4 * e + a) for a in range(4)]
            for v in range(tiles):
                weak = laplace([values[a][v] for a in range(4)], e, v)
                keep(1, lap2, f, e, v, weak)
        for copy in edge_copies(1, lap2, f):
            copy.start()
        return carry

    lax.fori_loop(0, nfield, second_pass, 0)

    def last_pass(f, carry):
        for copy in edge_copies(1, lap2, f):
            copy.wait_recv()
        for r in range(rows):
            done = assembled(1, lap2, f, r)
            for v in range(tiles):
                count = min(SUB, cols - v * SUB)
                result[f, r, pl.ds(v * SUB, count), :] = done[v][:count]
        pltpu.make_async_copy(result.at[f], out.at[f], store_sem.at[f]).start()
        return carry

    lax.fori_loop(0, nfield, last_pass, 0)

    def finish(f, carry):
        for copy in edge_copies(0, lap1, f) + edge_copies(1, lap2, f):
            copy.wait_send()
        pltpu.make_async_copy(result.at[f], out.at[f], store_sem.at[f]).wait()
        return carry

    for copy in mass_copies:
        copy.wait_send()
    lax.fori_loop(0, nfield, finish, 0)


def solution(mesh):
    faces, cols_axis = mesh.shape["face"], mesh.shape["col"]

    def shards(fields, metric_diag, metric_cross, point_mass):
        nfield, rows, cols, lanes = fields.shape
        wide = -(-cols // SUB) * SUB
        f32 = jnp.float32
        anywhere = pl.BlockSpec(memory_space=pl.ANY)
        return pl.pallas_call(
            functools.partial(operator_kernel, faces, cols_axis, nfield, rows, cols),
            out_shape=jax.ShapeDtypeStruct(fields.shape, f32),
            in_specs=[anywhere] * 4,
            out_specs=anywhere,
            scratch_shapes=[
                pltpu.VMEM((nfield, rows, cols, lanes), f32),
                pltpu.VMEM((2, rows, cols), f32),
                pltpu.VMEM((rows, cols), f32),
                pltpu.VMEM((rows, cols), f32),
                pltpu.VMEM((wide, LANES), f32),
                pltpu.VMEM((2, SUB, LANES), f32),
                pltpu.VMEM((2, wide, LANES), f32),
                pltpu.VMEM((4, SUB, LANES), f32),
                pltpu.VMEM((4, rows, wide, LANES), f32),
                pltpu.VMEM((nfield, rows + 2, wide, lanes), f32),
                pltpu.VMEM((nfield, rows + 2, wide, lanes), f32),
                pltpu.VMEM((2, nfield, rows, 1, lanes), f32),
                pltpu.VMEM((2, nfield, rows, 1, lanes), f32),
                pltpu.VMEM((2, nfield, rows + 2, 1, lanes), f32),
                pltpu.VMEM((2, nfield, rows + 2, 1, lanes), f32),
                pltpu.VMEM((nfield, rows, cols, lanes), f32),
                pltpu.SemaphoreType.DMA((nfield + 3,)),
                pltpu.SemaphoreType.DMA((nfield,)),
                pltpu.SemaphoreType.DMA((8,)),
                pltpu.SemaphoreType.DMA((8,)),
                pltpu.SemaphoreType.DMA((2, 8, nfield)),
                pltpu.SemaphoreType.DMA((2, 8, nfield)),
            ],
            compiler_params=pltpu.CompilerParams(collective_id=0, has_side_effects=True),
        )(fields, metric_diag, metric_cross, point_mass)

    return jax.shard_map(
        shards,
        mesh=mesh,
        in_specs=(
            P(None, "face", "col", None),
            P(None, "face", "col"),
            P("face", "col"),
            P("face", "col"),
        ),
        out_specs=P(None, "face", "col", None),
        check_vma=False,
    )
```

```python
import functools

import jax
import jax.numpy as jnp
import numpy as np
from jax import lax
from jax.experimental import pallas as pl
from jax.experimental.pallas import tpu as pltpu
from jax.sharding import PartitionSpec as P

MESH = pl.DeviceIdType.MESH
SUB = 8
LANES = 128


def derivative_table():
    small = 1.0 / np.sqrt(5.0)
    nodes = np.array([-1.0, -small, small, 1.0])
    count = nodes.shape[0]
    weights = np.array(
        [np.prod([nodes[a] - nodes[k] for k in range(count) if k != a]) for a in range(count)]
    )
    table = np.zeros((count, count))
    for a in range(count):
        for b in range(count):
            if a == b:
                table[a, b] = np.sum([1.0 / (nodes[a] - nodes[k]) for k in range(count) if k != a])
            else:
                table[a, b] = weights[a] / weights[b] / (nodes[a] - nodes[b])
    table[np.abs(table) < 1e-12] = 0.0
    return table


def combine(table, parts):
    out = []
    for a in range(4):
        total = None
        for b in range(4):
            if table[a, b] == 0.0:
                continue
            term = np.float32(table[a, b]) * parts[b]
            total = term if total is None else total + term
        out.append(total)
    return out


def pair_coefficients(table):
    high = lax.broadcasted_iota(jnp.int32, (SUB, LANES), 0) >= SUB // 2
    result = []
    for p in range(2):
        line = []
        for q in range(2):
            kept = jnp.where(high, np.float32(table[2 * p + 1, 2 * q + 1]), np.float32(table[2 * p, 2 * q]))
            swapped = jnp.where(high, np.float32(table[2 * p + 1, 2 * q]), np.float32(table[2 * p, 2 * q + 1]))
            line.append((kept, swapped))
        result.append(line)
    return result


def swap(tile):
    return pltpu.roll(tile, SUB // 2, 0)


def along(pair, coefficients):
    turned = [swap(x) for x in pair]
    out = []
    for p in range(2):
        total = None
        for q in range(2):
            kept, swapped = coefficients[p][q]
            term = kept * pair[q] + swapped * turned[q]
            total = term if total is None else total + term
        out.append(total)
    return out


def operator_kernel(
    faces, cols_axis, rows, cols,
    fields, diag, cross, mass,
    out,
    u, md, mc, mp, mpad, mrow, mside, mcorner, column, weights, lap1, lap2,
    load_sem, mass_send, mass_recv, edge_send, edge_recv,
):
    table = derivative_table()
    blocks_x, blocks_y = rows // 4, cols // 4
    pairs = cols // 2
    wide = -(-cols // SUB) * SUB
    face = lax.axis_index("face")
    col = lax.axis_index("col")
    up, down = lax.rem(face + faces - 1, faces), lax.rem(face + 1, faces)
    left, right = lax.rem(col + cols_axis - 1, cols_axis), lax.rem(col + 1, cols_axis)
    partners = (
        (up, col), (down, col), (face, left), (face, right),
        (up, left), (up, right), (down, left), (down, right),
    )

    barrier = pltpu.get_barrier_semaphore()
    for partner in partners:
        pl.semaphore_signal(barrier, inc=1, device_id=partner, device_id_type=MESH)

    small_loads = [
        pltpu.make_async_copy(source, target, load_sem.at[blocks_x + k])
        for k, (source, target) in enumerate(((diag, md), (cross, mc), (mass, mp)))
    ]

    def field_load(e):
        window = pl.ds(4 * e, 4)
        return pltpu.make_async_copy(fields.at[window], u.at[window], load_sem.at[e])

    for load in small_loads:
        load.start()
    for e in range(blocks_x):
        field_load(e).start()

    high = lax.broadcasted_iota(jnp.int32, (SUB, LANES), 0) >= SUB // 2

    def spread(k, square):
        turned = jnp.transpose(square)
        for r in range(rows):
            column[k, r] = jnp.broadcast_to(turned[:wide, r : r + 1], (wide, LANES))

        def pair_up(r, carry):
            for p in range(pairs):
                one = jnp.broadcast_to(column[k, r, pl.ds(2 * p, 1), :], (SUB, LANES))
                two = jnp.broadcast_to(column[k, r, pl.ds(2 * p + 1, 1), :], (SUB, LANES))
                weights[k, r, p] = jnp.where(high, two, one)
            return carry

        lax.fori_loop(0, rows, pair_up, 0)

    def padded(value):
        return lax.pad(value, np.float32(0), ((0, LANES - rows, 0), (0, LANES - cols, 0)))

    for load in small_loads:
        load.wait()
    mpad[...] = padded(mp[...])[:wide]
    spread(0, padded(md[:, 0, :]))
    spread(1, padded(md[:, 1, :]))
    spread(2, padded(mc[...]))

    forward = pair_coefficients(table)
    backward = pair_coefficients(table.T)

    def laplace(values, e, g):
        grad_x = [combine(table, [values[a][q] for a in range(4)]) for q in range(2)]
        flux_x, flux_y = [[], []], []
        for a in range(4):
            grad_y = along(values[a], forward)
            line = []
            for q in range(2):
                first, second, mixed = (weights[k, 4 * e + a, 2 * g + q] for k in range(3))
                flux_x[q].append(first * grad_x[q][a] + mixed * grad_y[q])
                line.append(mixed * grad_x[q][a] + second * grad_y[q])
            flux_y.append(line)
        weak = [combine(table.T, flux_x[q]) for q in range(2)]
        for a in range(4):
            other = along(flux_y[a], backward)
            for q in range(2):
                weak[q][a] = weak[q][a] + other[q]
        return weak

    def keep(lap, e, g, weak):
        for a in range(4):
            for q in range(2):
                lap[4 * e + a + 1, 2 * g + q + 1] = weak[q][a]

    half = SUB // 2
    low_half, high_half = pl.ds(0, half), pl.ds(half, half)

    def edge_copies(phase, lap):
        inner, across = pl.ds(1, rows), pl.ds(1, pairs)
        moves = (
            (lap.at[1, across], lap.at[rows + 1, across]),
            (lap.at[rows, across], lap.at[0, across]),
            (lap.at[inner, 1, low_half], lap.at[inner, pairs + 1, low_half]),
            (lap.at[inner, pairs, high_half], lap.at[inner, 0, high_half]),
            (lap.at[1, 1, low_half], lap.at[rows + 1, pairs + 1, low_half]),
            (lap.at[1, pairs, high_half], lap.at[rows + 1, 0, high_half]),
            (lap.at[rows, 1, low_half], lap.at[0, pairs + 1, low_half]),
            (lap.at[rows, pairs, high_half], lap.at[0, 0, high_half]),
        )
        return [
            pltpu.make_async_remote_copy(
                src_ref=source,
                dst_ref=target,
                send_sem=edge_send.at[phase, k],
                recv_sem=edge_recv.at[phase, k],
                device_id=partners[k],
                device_id_type=MESH,
            )
            for k, (source, target) in enumerate(moves)
        ]

    top, bottom = mpad.at[pl.ds(0, SUB)], mpad.at[pl.ds(wide - SUB, SUB)]
    mass_moves = (
        (top, mrow.at[1]), (bottom, mrow.at[0]),
        (mpad, mside.at[1]), (mpad, mside.at[0]),
        (top, mcorner.at[3]), (top, mcorner.at[2]),
        (bottom, mcorner.at[1]), (bottom, mcorner.at[0]),
    )
    mass_copies = [
        pltpu.make_async_remote_copy(
            src_ref=source,
            dst_ref=target,
            send_sem=mass_send.at[k],
            recv_sem=mass_recv.at[k],
            device_id=partners[k],
            device_id_type=MESH,
        )
        for k, (source, target) in enumerate(mass_moves)
    ]

    def first_pass(e, carry):
        field_load(e).wait()
        for g in range(blocks_y):
            values = [[u[4 * e + a, 2 * g + q] for q in range(2)] for a in range(4)]
            keep(lap1, e, g, laplace(values, e, g))
        return carry

    lax.fori_loop(0, blocks_x, first_pass, 0)

    pl.semaphore_wait(barrier, 8)
    first_copies = edge_copies(0, lap1)
    for copy in mass_copies + first_copies:
        copy.start()

    for copy in mass_copies:
        copy.wait_recv()
    rid = lax.broadcasted_iota(jnp.int32, (wide, LANES), 0)
    cid = lax.broadcasted_iota(jnp.int32, (wide, LANES), 1)
    zero = jnp.zeros((wide, LANES), jnp.float32)

    def down_rows(centre, north, south):
        total = centre
        inner_low = (rid % 4 == 0) & (rid > 0)
        inner_high = (rid % 4 == 3) & (rid < rows - 1)
        total = total + jnp.where(inner_low, pltpu.roll(centre, 1, 0), zero)
        total = total + jnp.where(inner_high, pltpu.roll(centre, wide - 1, 0), zero)
        before = jnp.broadcast_to(north, (wide, LANES))
        after = jnp.broadcast_to(south, (wide, LANES))
        total = total + jnp.where(rid == 0, before, zero)
        return total + jnp.where(rid == rows - 1, after, zero)

    last = (rows - 1) % SUB
    own = down_rows(mpad[...], mrow[0, last : last + 1], mrow[1, 0:1])
    west = down_rows(mside[0], mcorner[0, last : last + 1], mcorner[2, 0:1])
    east = down_rows(mside[1], mcorner[1, last : last + 1], mcorner[3, 0:1])
    total = own
    total = total + jnp.where((cid % 4 == 0) & (cid > 0), pltpu.roll(own, 1, 1), zero)
    total = total + jnp.where((cid % 4 == 3) & (cid < cols - 1), pltpu.roll(own, LANES - 1, 1), zero)
    total = total + jnp.where(cid == 0, pltpu.roll(west, LANES - cols + 1, 1), zero)
    total = total + jnp.where(cid == cols - 1, pltpu.roll(east, cols - 1, 1), zero)
    valid = (rid < rows) & (cid < cols)
    inverse = jnp.where(valid, 1.0 / jnp.where(valid, total, 1.0), 0.0)
    spread(3, jnp.concatenate([inverse, jnp.zeros((LANES - wide, LANES), jnp.float32)], axis=0))

    def assembled(lap, e, a):
        r = 4 * e + a
        parts = [lap[r + 1, p] for p in range(pairs + 2)]
        if a == 0:
            parts = [parts[p] + lap[r, p] for p in range(pairs + 2)]
        if a == 3:
            parts = [parts[p] + lap[r + 2, p] for p in range(pairs + 2)]
        tiles = []
        for p in range(pairs):
            if p % 2 == 0:
                add = jnp.where(high, 0.0, swap(parts[p]))
            else:
                add = jnp.where(high, swap(parts[p + 2]), 0.0)
            tiles.append((parts[p + 1] + add) * weights[3, r, p])
        return tiles

    for copy in first_copies:
        copy.wait_recv()

    def second_pass(e, carry):
        values = [assembled(lap1, e, a) for a in range(4)]
        for g in range(blocks_y):
            keep(lap2, e, g, laplace([[values[a][2 * g + q] for q in range(2)] for a in range(4)], e, g))
        return carry

    lax.fori_loop(0, blocks_x, second_pass, 0)

    second_copies = edge_copies(1, lap2)
    for copy in second_copies:
        copy.start()
    for copy in second_copies:
        copy.wait_recv()

    def last_pass(e, carry):
        for a in range(4):
            done = assembled(lap2, e, a)
            for p in range(pairs):
                out[4 * e + a, p] = done[p]
        return carry

    lax.fori_loop(0, blocks_x, last_pass, 0)

    for copy in mass_copies + first_copies + second_copies:
        copy.wait_send()


def solution(mesh):
    faces, cols_axis = mesh.shape["face"], mesh.shape["col"]

    def shards(fields, metric_diag, metric_cross, point_mass):
        nfield, rows, cols, lanes = fields.shape
        wide = -(-cols // SUB) * SUB
        pairs = cols // 2
        f32 = jnp.float32
        anywhere = pl.BlockSpec(memory_space=pl.ANY)
        tiles = fields.transpose(1, 2, 0, 3).reshape(rows, pairs, 2 * nfield, lanes)
        result = pl.pallas_call(
            functools.partial(operator_kernel, faces, cols_axis, rows, cols),
            out_shape=pltpu.VMEM((rows, pairs, 2 * nfield, lanes), f32),
            in_specs=[anywhere] * 4,
            out_specs=pl.BlockSpec(memory_space=pltpu.VMEM),
            scratch_shapes=[
                pltpu.VMEM((rows, pairs, SUB, lanes), f32),
                pltpu.VMEM((rows, 2, cols), f32),
                pltpu.VMEM((rows, cols), f32),
                pltpu.VMEM((rows, cols), f32),
                pltpu.VMEM((wide, LANES), f32),
                pltpu.VMEM((2, SUB, LANES), f32),
                pltpu.VMEM((2, wide, LANES), f32),
                pltpu.VMEM((4, SUB, LANES), f32),
                pltpu.VMEM((4, rows, wide, LANES), f32),
                pltpu.VMEM((4, rows, pairs, SUB, LANES), f32),
                pltpu.VMEM((rows + 2, pairs + 2, SUB, lanes), f32),
                pltpu.VMEM((rows + 2, pairs + 2, SUB, lanes), f32),
                pltpu.SemaphoreType.DMA((rows // 4 + 3,)),
                pltpu.SemaphoreType.DMA((8,)),
                pltpu.SemaphoreType.DMA((8,)),
                pltpu.SemaphoreType.DMA((2, 8)),
                pltpu.SemaphoreType.DMA((2, 8)),
            ],
            compiler_params=pltpu.CompilerParams(collective_id=0, has_side_effects=True),
        )(tiles, metric_diag.transpose(1, 0, 2), metric_cross, point_mass)
        return result.reshape(rows, cols, nfield, lanes).transpose(2, 0, 1, 3)

    return jax.shard_map(
        shards,
        mesh=mesh,
        in_specs=(
            P(None, "face", "col", None),
            P(None, "face", "col"),
            P("face", "col"),
            P("face", "col"),
        ),
        out_specs=P(None, "face", "col", None),
        check_vma=False,
    )
```

```python
import functools

import jax
import jax.numpy as jnp
import numpy as np
from jax import lax
from jax.experimental import pallas as pl
from jax.experimental.pallas import tpu as pltpu
from jax.sharding import PartitionSpec as P

MESH = pl.DeviceIdType.MESH
SUB = 8
LANES = 128


def derivative_table():
    small = 1.0 / np.sqrt(5.0)
    nodes = np.array([-1.0, -small, small, 1.0])
    count = nodes.shape[0]
    weights = np.array(
        [np.prod([nodes[a] - nodes[k] for k in range(count) if k != a]) for a in range(count)]
    )
    table = np.zeros((count, count))
    for a in range(count):
        for b in range(count):
            if a == b:
                table[a, b] = np.sum([1.0 / (nodes[a] - nodes[k]) for k in range(count) if k != a])
            else:
                table[a, b] = weights[a] / weights[b] / (nodes[a] - nodes[b])
    table[np.abs(table) < 1e-12] = 0.0
    return table


def combine(table, parts):
    out = []
    for a in range(4):
        total = None
        for b in range(4):
            if table[a, b] == 0.0:
                continue
            term = np.float32(table[a, b]) * parts[b]
            total = term if total is None else total + term
        out.append(total)
    return out


def pair_coefficients(table):
    high = lax.broadcasted_iota(jnp.int32, (SUB, LANES), 0) >= SUB // 2
    result = []
    for p in range(2):
        line = []
        for q in range(2):
            kept = jnp.where(high, np.float32(table[2 * p + 1, 2 * q + 1]), np.float32(table[2 * p, 2 * q]))
            swapped = jnp.where(high, np.float32(table[2 * p + 1, 2 * q]), np.float32(table[2 * p, 2 * q + 1]))
            line.append((kept, swapped))
        result.append(line)
    return result


def swap(tile):
    return pltpu.roll(tile, SUB // 2, 0)


def along(pair, coefficients):
    turned = [swap(x) for x in pair]
    out = []
    for p in range(2):
        total = None
        for q in range(2):
            kept, swapped = coefficients[p][q]
            term = kept * pair[q] + swapped * turned[q]
            total = term if total is None else total + term
        out.append(total)
    return out


def operator_kernel(
    faces, cols_axis, rows, cols,
    fields, diag, cross, mass,
    out,
    u, md, mc, mp, mpad, mrow, mside, mcorner, column, weights, lap1, lap2,
    load_sem, mass_send, mass_recv, edge_send, edge_recv,
):
    table = derivative_table()
    blocks_x, blocks_y = rows // 4, cols // 4
    pairs = cols // 2
    wide = -(-cols // SUB) * SUB
    face = lax.axis_index("face")
    col = lax.axis_index("col")
    up, down = lax.rem(face + faces - 1, faces), lax.rem(face + 1, faces)
    left, right = lax.rem(col + cols_axis - 1, cols_axis), lax.rem(col + 1, cols_axis)
    partners = (
        (up, col), (down, col), (face, left), (face, right),
        (up, left), (up, right), (down, left), (down, right),
    )

    barrier = pltpu.get_barrier_semaphore()
    for partner in partners:
        pl.semaphore_signal(barrier, inc=1, device_id=partner, device_id_type=MESH)

    small_loads = [
        pltpu.make_async_copy(source, target, load_sem.at[blocks_x + k])
        for k, (source, target) in enumerate(((diag, md), (cross, mc), (mass, mp)))
    ]

    def field_load(e):
        window = pl.ds(4 * e, 4)
        return pltpu.make_async_copy(fields.at[window], u.at[window], load_sem.at[e])

    for load in small_loads:
        load.start()
    for e in range(blocks_x):
        field_load(e).start()

    high = lax.broadcasted_iota(jnp.int32, (SUB, LANES), 0) >= SUB // 2

    def pair_tile(k, r, p):
        one = jnp.broadcast_to(column[k, r, pl.ds(2 * p, 1), :], (SUB, LANES))
        two = jnp.broadcast_to(column[k, r, pl.ds(2 * p + 1, 1), :], (SUB, LANES))
        weights[k, r, p] = jnp.where(high, two, one)

    def spread(k, turned):
        for r in range(rows):
            column[k, r] = jnp.broadcast_to(turned[:, r : r + 1], (wide, LANES))

        def pair_up(r, carry):
            for p in range(pairs):
                pair_tile(k, r, p)
            return carry

        lax.fori_loop(0, rows, pair_up, 0)

    def turned(value):
        square = lax.pad(value, np.float32(0), ((0, LANES - rows, 0), (0, LANES - cols, 0)))
        return jnp.transpose(square)[:wide]

    cid = lax.broadcasted_iota(jnp.int32, (wide, LANES), 0)
    rid = lax.broadcasted_iota(jnp.int32, (wide, LANES), 1)
    zero = jnp.zeros((wide, LANES), jnp.float32)
    valid = (rid < rows) & (cid < cols)

    def over_columns(centre):
        total = centre + jnp.where((cid % 4 == 0) & (cid > 0), pltpu.roll(centre, 1, 0), zero)
        return total + jnp.where((cid % 4 == 3) & (cid < cols - 1), pltpu.roll(centre, wide - 1, 0), zero)

    def over_rows(centre):
        total = centre + jnp.where((rid % 4 == 0) & (rid > 0), pltpu.roll(centre, 1, 1), zero)
        return total + jnp.where((rid % 4 == 3) & (rid < rows - 1), pltpu.roll(centre, LANES - 1, 1), zero)

    def inverse(total):
        return jnp.where(valid, 1.0 / jnp.where(valid, total, 1.0), 0.0)

    for load in small_loads:
        load.wait()
    mpad[...] = turned(mp[...])
    spread(0, turned(md[:, 0, :]))
    spread(1, turned(md[:, 1, :]))
    spread(2, turned(mc[...]))

    forward = pair_coefficients(table)
    backward = pair_coefficients(table.T)

    def laplace(values, e, g):
        grad_x = [combine(table, [values[a][q] for a in range(4)]) for q in range(2)]
        flux_x, flux_y = [[], []], []
        for a in range(4):
            grad_y = along(values[a], forward)
            line = []
            for q in range(2):
                first, second, mixed = (weights[k, 4 * e + a, 2 * g + q] for k in range(3))
                flux_x[q].append(first * grad_x[q][a] + mixed * grad_y[q])
                line.append(mixed * grad_x[q][a] + second * grad_y[q])
            flux_y.append(line)
        weak = [combine(table.T, flux_x[q]) for q in range(2)]
        for a in range(4):
            other = along(flux_y[a], backward)
            for q in range(2):
                weak[q][a] = weak[q][a] + other[q]
        return weak

    def keep(lap, e, g, weak):
        for a in range(4):
            for q in range(2):
                lap[4 * e + a + 1, 2 * g + q + 1] = weak[q][a]

    half = SUB // 2
    low_half, high_half = pl.ds(0, half), pl.ds(half, half)

    def remote(source, target, k, send_sem, recv_sem):
        return pltpu.make_async_remote_copy(
            src_ref=source,
            dst_ref=target,
            send_sem=send_sem,
            recv_sem=recv_sem,
            device_id=partners[k],
            device_id_type=MESH,
        )

    def edge_copies(phase, lap):
        inner, across = pl.ds(1, rows), pl.ds(1, pairs)
        moves = (
            (lap.at[1, across], lap.at[rows + 1, across]),
            (lap.at[rows, across], lap.at[0, across]),
            (lap.at[inner, 1, low_half], lap.at[inner, pairs + 1, low_half]),
            (lap.at[inner, pairs, high_half], lap.at[inner, 0, high_half]),
            (lap.at[1, 1, low_half], lap.at[rows + 1, pairs + 1, low_half]),
            (lap.at[1, pairs, high_half], lap.at[rows + 1, 0, high_half]),
            (lap.at[rows, 1, low_half], lap.at[0, pairs + 1, low_half]),
            (lap.at[rows, pairs, high_half], lap.at[0, 0, high_half]),
        )
        return [
            remote(source, target, k, edge_send.at[phase, k], edge_recv.at[phase, k])
            for k, (source, target) in enumerate(moves)
        ]

    left_tile, right_tile = mpad.at[pl.ds(0, SUB)], mpad.at[pl.ds(wide - SUB, SUB)]
    mass_moves = (
        (mpad, mside.at[1]), (mpad, mside.at[0]),
        (left_tile, mrow.at[1]), (right_tile, mrow.at[0]),
        (left_tile, mcorner.at[3]), (right_tile, mcorner.at[2]),
        (left_tile, mcorner.at[1]), (right_tile, mcorner.at[0]),
    )
    mass_copies = [
        remote(source, target, k, mass_send.at[k], mass_recv.at[k])
        for k, (source, target) in enumerate(mass_moves)
    ]

    def first_pass(e, carry):
        field_load(e).wait()
        for g in range(blocks_y):
            values = [[u[4 * e + a, 2 * g + q] for q in range(2)] for a in range(4)]
            keep(lap1, e, g, laplace(values, e, g))
        return carry

    lax.fori_loop(0, blocks_x, first_pass, 0)

    spread(3, inverse(over_rows(over_columns(mpad[...]))))

    pl.semaphore_wait(barrier, 8)
    first_copies = edge_copies(0, lap1)
    for copy in first_copies[4:] + mass_copies[4:] + mass_copies[2:4] + first_copies[2:4] + mass_copies[:2] + first_copies[:2]:
        copy.start()

    def assembled(lap, e, a, window):
        r = 4 * e + a

        def summed(p):
            part = lap[r + 1, p + 1]
            if a == 0:
                part = part + lap[r, p + 1]
            if a == 3:
                part = part + lap[r + 2, p + 1]
            return part

        parts = {}
        tiles = []
        for p in window:
            other = p - 1 if p % 2 == 0 else p + 1
            for q in (p, other):
                if q not in parts:
                    parts[q] = summed(q)
            turn = swap(parts[other])
            add = jnp.where(high, 0.0, turn) if p % 2 == 0 else jnp.where(high, turn, 0.0)
            tiles.append((parts[p] + add) * weights[3, r, p])
        return tiles

    def second(e, g):
        values = [assembled(lap1, e, a, (2 * g, 2 * g + 1)) for a in range(4)]
        keep(lap2, e, g, laplace(values, e, g))

    inner_blocks = range(1, blocks_y - 1)
    rim_blocks = (0, blocks_y - 1)

    def loop(low, high_end, body):
        def step(i, carry):
            body(i)
            return carry

        lax.fori_loop(low, high_end, step, 0)

    def over(blocks):
        def body(e):
            for g in blocks:
                second(e, g)

        return body

    loop(1, blocks_x - 1, over(inner_blocks))

    for copy in mass_copies:
        copy.wait_recv()

    def with_ends(centre, before, after):
        total = over_columns(centre)
        total = total + jnp.where(cid == 0, jnp.broadcast_to(before, (wide, LANES)), zero)
        return total + jnp.where(cid == cols - 1, jnp.broadcast_to(after, (wide, LANES)), zero)

    last = (cols - 1) % SUB
    own = with_ends(mpad[...], mrow[0, last : last + 1], mrow[1, 0:1])
    north = with_ends(mside[0], mcorner[0, last : last + 1], mcorner[1, 0:1])
    south = with_ends(mside[1], mcorner[2, last : last + 1], mcorner[3, 0:1])
    total = over_rows(own)
    total = total + jnp.where(rid == 0, pltpu.roll(north, LANES - rows + 1, 1), zero)
    total = total + jnp.where(rid == rows - 1, pltpu.roll(south, rows - 1, 1), zero)
    full = inverse(total)
    for r in range(rows):
        if r in (0, rows - 1):
            column[3, r] = jnp.broadcast_to(full[:, r : r + 1], (wide, LANES))
            for p in range(pairs):
                pair_tile(3, r, p)
        else:
            for p in (0, pairs - 1):
                start = 2 * p // SUB * SUB
                column[3, r, pl.ds(start, SUB), :] = jnp.broadcast_to(full[start : start + SUB, r : r + 1], (SUB, LANES))
                pair_tile(3, r, p)

    for copy in first_copies:
        copy.wait_recv()

    second_copies = edge_copies(1, lap2)
    loop(0, 2, lambda i: over(rim_blocks)(i * (blocks_x - 1)))
    for copy in second_copies[4:]:
        copy.start()
    loop(1, blocks_x - 1, over(rim_blocks))
    for copy in second_copies[2:4]:
        copy.start()
    loop(0, 2, lambda i: over(inner_blocks)(i * (blocks_x - 1)))
    for copy in second_copies[:2]:
        copy.start()

    def write(e, a, window):
        for p, tile in zip(window, assembled(lap2, e, a, window)):
            out[4 * e + a, p] = tile

    middle, rim = tuple(range(1, pairs - 1)), (0, pairs - 1)

    def write_rows(window):
        for a in range(1, 4):
            write(0, a, window)
        for a in range(3):
            write(blocks_x - 1, a, window)

        def body(e):
            for a in range(4):
                write(e, a, window)

        loop(1, blocks_x - 1, body)

    write_rows(middle)
    for copy in second_copies:
        copy.wait_recv()
    write_rows(rim)
    write(0, 0, tuple(range(pairs)))
    write(blocks_x - 1, 3, tuple(range(pairs)))

    for copy in mass_copies + first_copies + second_copies:
        copy.wait_send()


def solution(mesh):
    faces, cols_axis = mesh.shape["face"], mesh.shape["col"]

    def shards(fields, metric_diag, metric_cross, point_mass):
        nfield, rows, cols, lanes = fields.shape
        wide = -(-cols // SUB) * SUB
        pairs = cols // 2
        f32 = jnp.float32
        anywhere = pl.BlockSpec(memory_space=pl.ANY)
        tiles = fields.transpose(1, 2, 0, 3).reshape(rows, pairs, 2 * nfield, lanes)
        result = pl.pallas_call(
            functools.partial(operator_kernel, faces, cols_axis, rows, cols),
            out_shape=pltpu.VMEM((rows, pairs, 2 * nfield, lanes), f32),
            in_specs=[anywhere] * 4,
            out_specs=pl.BlockSpec(memory_space=pltpu.VMEM),
            scratch_shapes=[
                pltpu.VMEM((rows, pairs, SUB, lanes), f32),
                pltpu.VMEM((rows, 2, cols), f32),
                pltpu.VMEM((rows, cols), f32),
                pltpu.VMEM((rows, cols), f32),
                pltpu.VMEM((wide, LANES), f32),
                pltpu.VMEM((2, SUB, LANES), f32),
                pltpu.VMEM((2, wide, LANES), f32),
                pltpu.VMEM((4, SUB, LANES), f32),
                pltpu.VMEM((4, rows, wide, LANES), f32),
                pltpu.VMEM((4, rows, pairs, SUB, LANES), f32),
                pltpu.VMEM((rows + 2, pairs + 2, SUB, lanes), f32),
                pltpu.VMEM((rows + 2, pairs + 2, SUB, lanes), f32),
                pltpu.SemaphoreType.DMA((rows // 4 + 3,)),
                pltpu.SemaphoreType.DMA((8,)),
                pltpu.SemaphoreType.DMA((8,)),
                pltpu.SemaphoreType.DMA((2, 8)),
                pltpu.SemaphoreType.DMA((2, 8)),
            ],
            compiler_params=pltpu.CompilerParams(collective_id=0, has_side_effects=True),
        )(tiles, metric_diag.transpose(1, 0, 2), metric_cross, point_mass)
        return result.reshape(rows, cols, nfield, lanes).transpose(2, 0, 1, 3)

    return jax.shard_map(
        shards,
        mesh=mesh,
        in_specs=(
            P(None, "face", "col", None),
            P(None, "face", "col"),
            P("face", "col"),
            P("face", "col"),
        ),
        out_specs=P(None, "face", "col", None),
        check_vma=False,
    )
```

```python
import functools

import jax
import jax.numpy as jnp
import numpy as np
from jax import lax
from jax.experimental import pallas as pl
from jax.experimental.pallas import tpu as pltpu
from jax.sharding import PartitionSpec as P

MESH = pl.DeviceIdType.MESH
SUB = 8
LANES = 128


def derivative_table():
    small = 1.0 / np.sqrt(5.0)
    nodes = np.array([-1.0, -small, small, 1.0])
    count = nodes.shape[0]
    weights = np.array(
        [np.prod([nodes[a] - nodes[k] for k in range(count) if k != a]) for a in range(count)]
    )
    table = np.zeros((count, count))
    for a in range(count):
        for b in range(count):
            if a == b:
                table[a, b] = np.sum([1.0 / (nodes[a] - nodes[k]) for k in range(count) if k != a])
            else:
                table[a, b] = weights[a] / weights[b] / (nodes[a] - nodes[b])
    table[np.abs(table) < 1e-12] = 0.0
    return table


def combine(table, parts):
    out = []
    for a in range(4):
        total = None
        for b in range(4):
            if table[a, b] == 0.0:
                continue
            term = np.float32(table[a, b]) * parts[b]
            total = term if total is None else total + term
        out.append(total)
    return out


def pair_coefficients(table):
    high = lax.broadcasted_iota(jnp.int32, (SUB, LANES), 0) >= SUB // 2
    result = []
    for p in range(2):
        line = []
        for q in range(2):
            kept = jnp.where(high, np.float32(table[2 * p + 1, 2 * q + 1]), np.float32(table[2 * p, 2 * q]))
            swapped = jnp.where(high, np.float32(table[2 * p + 1, 2 * q]), np.float32(table[2 * p, 2 * q + 1]))
            line.append((kept, swapped))
        result.append(line)
    return result


def swap(tile):
    return pltpu.roll(tile, SUB // 2, 0)


def along(pair, coefficients):
    turned = [swap(x) for x in pair]
    out = []
    for p in range(2):
        total = None
        for q in range(2):
            kept, swapped = coefficients[p][q]
            term = kept * pair[q] + swapped * turned[q]
            total = term if total is None else total + term
        out.append(total)
    return out


def operator_kernel(
    faces, cols_axis, rows, cols,
    fields, diag, cross, mass,
    out,
    u, md, mc, mp, mpad, mrow, mside, mcorner, column, weights, lap1, lap2,
    load_sem, mass_send, mass_recv, edge_send, edge_recv,
):
    table = derivative_table()
    blocks_x, blocks_y = rows // 4, cols // 4
    pairs = cols // 2
    wide = -(-cols // SUB) * SUB
    face = lax.axis_index("face")
    col = lax.axis_index("col")
    up, down = lax.rem(face + faces - 1, faces), lax.rem(face + 1, faces)
    left, right = lax.rem(col + cols_axis - 1, cols_axis), lax.rem(col + 1, cols_axis)
    partners = (
        (up, col), (down, col), (face, left), (face, right),
        (up, left), (up, right), (down, left), (down, right),
    )

    barrier = pltpu.get_barrier_semaphore()
    for partner in partners:
        pl.semaphore_signal(barrier, inc=1, device_id=partner, device_id_type=MESH)

    small_loads = [
        pltpu.make_async_copy(source, target, load_sem.at[blocks_x + k])
        for k, (source, target) in enumerate(((diag, md), (cross, mc), (mass, mp)))
    ]

    def field_load(e):
        window = pl.ds(4 * e, 4)
        return pltpu.make_async_copy(fields.at[window], u.at[window], load_sem.at[e])

    for load in small_loads:
        load.start()
    for e in range(blocks_x):
        field_load(e).start()

    high = lax.broadcasted_iota(jnp.int32, (SUB, LANES), 0) >= SUB // 2

    def pair_tile(k, r, p):
        one = jnp.broadcast_to(column[k, r, pl.ds(2 * p, 1), :], (SUB, LANES))
        two = jnp.broadcast_to(column[k, r, pl.ds(2 * p + 1, 1), :], (SUB, LANES))
        weights[k, r, p] = jnp.where(high, two, one)

    def spread(k, turned):
        for r in range(rows):
            column[k, r] = jnp.broadcast_to(turned[:, r : r + 1], (wide, LANES))

        def pair_up(r, carry):
            for p in range(pairs):
                pair_tile(k, r, p)
            return carry

        lax.fori_loop(0, rows, pair_up, 0)

    def turned(value):
        square = lax.pad(value, np.float32(0), ((0, LANES - rows, 0), (0, LANES - cols, 0)))
        return jnp.transpose(square)[:wide]

    cid = lax.broadcasted_iota(jnp.int32, (wide, LANES), 0)
    rid = lax.broadcasted_iota(jnp.int32, (wide, LANES), 1)
    zero = jnp.zeros((wide, LANES), jnp.float32)
    valid = (rid < rows) & (cid < cols)

    def over_columns(centre):
        total = centre + jnp.where((cid % 4 == 0) & (cid > 0), pltpu.roll(centre, 1, 0), zero)
        return total + jnp.where((cid % 4 == 3) & (cid < cols - 1), pltpu.roll(centre, wide - 1, 0), zero)

    def over_rows(centre):
        total = centre + jnp.where((rid % 4 == 0) & (rid > 0), pltpu.roll(centre, 1, 1), zero)
        return total + jnp.where((rid % 4 == 3) & (rid < rows - 1), pltpu.roll(centre, LANES - 1, 1), zero)

    def inverse(total):
        return jnp.where(valid, 1.0 / jnp.where(valid, total, 1.0), 0.0)

    for load in small_loads:
        load.wait()
    mpad[...] = turned(mp[...])
    spread(0, turned(md[:, 0, :]))
    spread(1, turned(md[:, 1, :]))
    spread(2, turned(mc[...]))

    forward = pair_coefficients(table)
    backward = pair_coefficients(table.T)

    def laplace(values, e, g):
        grad_x = [combine(table, [values[a][q] for a in range(4)]) for q in range(2)]
        flux_x, flux_y = [[], []], []
        for a in range(4):
            grad_y = along(values[a], forward)
            line = []
            for q in range(2):
                first, second, mixed = (weights[k, 4 * e + a, 2 * g + q] for k in range(3))
                flux_x[q].append(first * grad_x[q][a] + mixed * grad_y[q])
                line.append(mixed * grad_x[q][a] + second * grad_y[q])
            flux_y.append(line)
        weak = [combine(table.T, flux_x[q]) for q in range(2)]
        for a in range(4):
            other = along(flux_y[a], backward)
            for q in range(2):
                weak[q][a] = weak[q][a] + other[q]
        return weak

    def keep(lap, e, g, weak):
        for a in range(4):
            for q in range(2):
                lap[4 * e + a + 1, 2 * g + q + 1] = weak[q][a]

    half = SUB // 2
    low_half, high_half = pl.ds(0, half), pl.ds(half, half)

    def remote(source, target, k, send_sem, recv_sem):
        return pltpu.make_async_remote_copy(
            src_ref=source,
            dst_ref=target,
            send_sem=send_sem,
            recv_sem=recv_sem,
            device_id=partners[k],
            device_id_type=MESH,
        )

    def edge_copies(phase, lap):
        inner, across = pl.ds(1, rows), pl.ds(1, pairs)
        moves = (
            (lap.at[1, across], lap.at[rows + 1, across]),
            (lap.at[rows, across], lap.at[0, across]),
            (lap.at[inner, 1, low_half], lap.at[inner, pairs + 1, low_half]),
            (lap.at[inner, pairs, high_half], lap.at[inner, 0, high_half]),
            (lap.at[1, 1, low_half], lap.at[rows + 1, pairs + 1, low_half]),
            (lap.at[1, pairs, high_half], lap.at[rows + 1, 0, high_half]),
            (lap.at[rows, 1, low_half], lap.at[0, pairs + 1, low_half]),
            (lap.at[rows, pairs, high_half], lap.at[0, 0, high_half]),
        )
        return [
            remote(source, target, k, edge_send.at[phase, k], edge_recv.at[phase, k])
            for k, (source, target) in enumerate(moves)
        ]

    def split_copies(lap):
        west_rows = (pl.ds(1, rows - 4), pl.ds(rows - 3, 4))
        east_rows = (pl.ds(5, rows - 4), pl.ds(1, 4))
        north_pairs = (pl.ds(1, pairs - 2), pl.ds(pairs - 1, 2))
        south_pairs = (pl.ds(3, pairs - 2), pl.ds(1, 2))
        pieces = []
        for n in range(2):
            line = (
                (lap.at[1, north_pairs[n]], lap.at[rows + 1, north_pairs[n]]),
                (lap.at[rows, south_pairs[n]], lap.at[0, south_pairs[n]]),
                (lap.at[west_rows[n], 1, low_half], lap.at[west_rows[n], pairs + 1, low_half]),
                (lap.at[east_rows[n], pairs, high_half], lap.at[east_rows[n], 0, high_half]),
            )
            pieces.append(
                [
                    remote(source, target, k, edge_send.at[1 + n, k], edge_recv.at[1 + n, k])
                    for k, (source, target) in enumerate(line)
                ]
            )
        return pieces

    left_tile, right_tile = mpad.at[pl.ds(0, SUB)], mpad.at[pl.ds(wide - SUB, SUB)]
    mass_moves = (
        (mpad, mside.at[1]), (mpad, mside.at[0]),
        (left_tile, mrow.at[1]), (right_tile, mrow.at[0]),
        (left_tile, mcorner.at[3]), (right_tile, mcorner.at[2]),
        (left_tile, mcorner.at[1]), (right_tile, mcorner.at[0]),
    )
    mass_copies = [
        remote(source, target, k, mass_send.at[k], mass_recv.at[k])
        for k, (source, target) in enumerate(mass_moves)
    ]

    def first_pass(e, carry):
        field_load(e).wait()
        for g in range(blocks_y):
            values = [[u[4 * e + a, 2 * g + q] for q in range(2)] for a in range(4)]
            keep(lap1, e, g, laplace(values, e, g))
        return carry

    lax.fori_loop(0, blocks_x, first_pass, 0)

    spread(3, inverse(over_rows(over_columns(mpad[...]))))

    pl.semaphore_wait(barrier, 8)
    first_copies = edge_copies(0, lap1)
    for copy in first_copies[4:] + mass_copies[4:] + mass_copies[2:4] + first_copies[2:4] + mass_copies[:2] + first_copies[:2]:
        copy.start()

    def assembled(lap, e, a, window):
        r = 4 * e + a

        def summed(p):
            part = lap[r + 1, p + 1]
            if a == 0:
                part = part + lap[r, p + 1]
            if a == 3:
                part = part + lap[r + 2, p + 1]
            return part

        parts = {}
        tiles = []
        for p in window:
            other = p - 1 if p % 2 == 0 else p + 1
            for q in (p, other):
                if q not in parts:
                    parts[q] = summed(q)
            turn = swap(parts[other])
            add = jnp.where(high, 0.0, turn) if p % 2 == 0 else jnp.where(high, turn, 0.0)
            tiles.append((parts[p] + add) * weights[3, r, p])
        return tiles

    def second(e, g):
        values = []
        for a in range(4):
            r = 4 * e + a
            parts = []
            for p in range(4):
                part = lap1[r + 1, 2 * g + p]
                if a == 0:
                    part = part + lap1[r, 2 * g + p]
                if a == 3:
                    part = part + lap1[r + 2, 2 * g + p]
                parts.append(part)
            left_tile = parts[1] + jnp.where(high, 0.0, swap(parts[0]))
            right_tile = parts[2] + jnp.where(high, swap(parts[3]), 0.0)
            values.append([left_tile * weights[3, r, 2 * g], right_tile * weights[3, r, 2 * g + 1]])
        keep(lap2, e, g, laplace(values, e, g))

    inner_blocks = range(1, blocks_y - 1)
    rim_blocks = (0, blocks_y - 1)

    def loop(low, high_end, body):
        def step(i, carry):
            body(i)
            return carry

        lax.fori_loop(low, high_end, step, 0)

    def over(blocks):
        def body(e):
            for g in blocks:
                second(e, g)

        return body

    inner_count = blocks_y - 2
    loop(0, (blocks_x - 2) * inner_count, lambda i: second(1 + i // inner_count, 1 + i % inner_count))

    def with_ends(centre, before, after):
        total = over_columns(centre)
        if before is not None:
            total = total + jnp.where(cid == 0, jnp.broadcast_to(before, (wide, LANES)), zero)
        if after is not None:
            total = total + jnp.where(cid == cols - 1, jnp.broadcast_to(after, (wide, LANES)), zero)
        return total

    def whole_inverse(north_east, south_west):
        own = with_ends(mpad[...], mrow[0, last : last + 1], mrow[1, 0:1])
        north = with_ends(mside[0], mcorner[0, last : last + 1], north_east)
        south = with_ends(mside[1], south_west, mcorner[3, 0:1])
        total = over_rows(own)
        total = total + jnp.where(rid == 0, pltpu.roll(north, LANES - rows + 1, 1), zero)
        return inverse(total + jnp.where(rid == rows - 1, pltpu.roll(south, rows - 1, 1), zero))

    def renew(full, r, p):
        start = 2 * p // SUB * SUB
        column[3, r, pl.ds(start, SUB), :] = jnp.broadcast_to(full[start : start + SUB, r : r + 1], (SUB, LANES))
        pair_tile(3, r, p)

    last = (cols - 1) % SUB
    near = (0, 1, 2, 3, 4, 7)
    for k in near:
        mass_copies[k].wait_recv()
    full = whole_inverse(None, None)
    for r in range(rows):
        if r in (0, rows - 1):
            column[3, r] = jnp.broadcast_to(full[:, r : r + 1], (wide, LANES))
            for p in range(pairs):
                pair_tile(3, r, p)
        else:
            for p in (0, pairs - 1):
                renew(full, r, p)

    second_copies = edge_copies(1, lap2)[4:]
    bulk, tip = split_copies(lap2)
    for k in near:
        first_copies[k].wait_recv()
    loop(0, 2, lambda i: second(i * (blocks_x - 1), i * (blocks_y - 1)))
    second_copies[0].start()
    second_copies[3].start()
    loop(0, 2 * (blocks_x - 2), lambda i: second(1 + i // 2, i % 2 * (blocks_y - 1)))
    bulk[2].start()
    bulk[3].start()
    for k in (5, 6):
        mass_copies[k].wait_recv()
    full = whole_inverse(mcorner[1, 0:1], mcorner[2, last : last + 1])
    renew(full, 0, pairs - 1)
    renew(full, rows - 1, 0)
    for k in (5, 6):
        first_copies[k].wait_recv()
    loop(0, 2, lambda i: second(i * (blocks_x - 1), (1 - i) * (blocks_y - 1)))
    for copy in second_copies[1:3] + tip[2:] + tip[:2]:
        copy.start()
    loop(0, 2 * inner_count, lambda i: second(i // inner_count * (blocks_x - 1), 1 + i % inner_count))
    bulk[0].start()
    bulk[1].start()
    second_copies = second_copies + bulk + tip

    def write(e, a, window):
        for p, tile in zip(window, assembled(lap2, e, a, window)):
            out[4 * e + a, p] = tile

    middle, rim = tuple(range(1, pairs - 1)), (0, pairs - 1)

    def write_rows(window):
        for a in range(1, 4):
            write(0, a, window)
        for a in range(3):
            write(blocks_x - 1, a, window)

        def body(e):
            for a in range(4):
                write(e, a, window)

        loop(1, blocks_x - 1, body)

    write_rows(middle)
    for copy in second_copies:
        copy.wait_recv()
    write_rows(rim)
    write(0, 0, tuple(range(pairs)))
    write(blocks_x - 1, 3, tuple(range(pairs)))

    for copy in mass_copies + first_copies + second_copies:
        copy.wait_send()


def solution(mesh):
    faces, cols_axis = mesh.shape["face"], mesh.shape["col"]

    def shards(fields, metric_diag, metric_cross, point_mass):
        nfield, rows, cols, lanes = fields.shape
        wide = -(-cols // SUB) * SUB
        pairs = cols // 2
        f32 = jnp.float32
        anywhere = pl.BlockSpec(memory_space=pl.ANY)
        tiles = fields.transpose(1, 2, 0, 3).reshape(rows, pairs, 2 * nfield, lanes)
        result = pl.pallas_call(
            functools.partial(operator_kernel, faces, cols_axis, rows, cols),
            out_shape=pltpu.VMEM((rows, pairs, 2 * nfield, lanes), f32),
            in_specs=[anywhere] * 4,
            out_specs=pl.BlockSpec(memory_space=pltpu.VMEM),
            scratch_shapes=[
                pltpu.VMEM((rows, pairs, SUB, lanes), f32),
                pltpu.VMEM((rows, 2, cols), f32),
                pltpu.VMEM((rows, cols), f32),
                pltpu.VMEM((rows, cols), f32),
                pltpu.VMEM((wide, LANES), f32),
                pltpu.VMEM((2, SUB, LANES), f32),
                pltpu.VMEM((2, wide, LANES), f32),
                pltpu.VMEM((4, SUB, LANES), f32),
                pltpu.VMEM((4, rows, wide, LANES), f32),
                pltpu.VMEM((4, rows, pairs, SUB, LANES), f32),
                pltpu.VMEM((rows + 2, pairs + 2, SUB, lanes), f32),
                pltpu.VMEM((rows + 2, pairs + 2, SUB, lanes), f32),
                pltpu.SemaphoreType.DMA((rows // 4 + 3,)),
                pltpu.SemaphoreType.DMA((8,)),
                pltpu.SemaphoreType.DMA((8,)),
                pltpu.SemaphoreType.DMA((3, 8)),
                pltpu.SemaphoreType.DMA((3, 8)),
            ],
            compiler_params=pltpu.CompilerParams(collective_id=0, has_side_effects=True),
        )(tiles, metric_diag.transpose(1, 0, 2), metric_cross, point_mass)
        return result.reshape(rows, cols, nfield, lanes).transpose(2, 0, 1, 3)

    return jax.shard_map(
        shards,
        mesh=mesh,
        in_specs=(
            P(None, "face", "col", None),
            P(None, "face", "col"),
            P("face", "col"),
            P("face", "col"),
        ),
        out_specs=P(None, "face", "col", None),
        check_vma=False,
    )
```

```python
import functools

import jax
import jax.numpy as jnp
import numpy as np
from jax import lax
from jax.experimental import pallas as pl
from jax.experimental.pallas import tpu as pltpu
from jax.sharding import PartitionSpec as P

MESH = pl.DeviceIdType.MESH
SUB = 8
LANES = 128


def derivative_table():
    small = 1.0 / np.sqrt(5.0)
    nodes = np.array([-1.0, -small, small, 1.0])
    count = nodes.shape[0]
    weights = np.array(
        [np.prod([nodes[a] - nodes[k] for k in range(count) if k != a]) for a in range(count)]
    )
    table = np.zeros((count, count))
    for a in range(count):
        for b in range(count):
            if a == b:
                table[a, b] = np.sum([1.0 / (nodes[a] - nodes[k]) for k in range(count) if k != a])
            else:
                table[a, b] = weights[a] / weights[b] / (nodes[a] - nodes[b])
    table[np.abs(table) < 1e-12] = 0.0
    return table


def combine(table, parts):
    out = []
    for a in range(4):
        total = None
        for b in range(4):
            if table[a, b] == 0.0:
                continue
            term = np.float32(table[a, b]) * parts[b]
            total = term if total is None else total + term
        out.append(total)
    return out


def pair_coefficients(table):
    high = lax.broadcasted_iota(jnp.int32, (SUB, LANES), 0) >= SUB // 2
    result = []
    for p in range(2):
        line = []
        for q in range(2):
            kept = jnp.where(high, np.float32(table[2 * p + 1, 2 * q + 1]), np.float32(table[2 * p, 2 * q]))
            swapped = jnp.where(high, np.float32(table[2 * p + 1, 2 * q]), np.float32(table[2 * p, 2 * q + 1]))
            line.append((kept, swapped))
        result.append(line)
    return result


def swap(tile):
    return pltpu.roll(tile, SUB // 2, 0)


def along(pair, coefficients):
    turned = [swap(x) for x in pair]
    out = []
    for p in range(2):
        total = None
        for q in range(2):
            kept, swapped = coefficients[p][q]
            term = kept * pair[q] + swapped * turned[q]
            total = term if total is None else total + term
        out.append(total)
    return out


def operator_kernel(
    faces, cols_axis, rows, cols,
    fields, diag, cross, mass,
    out,
    u, md, mc, mp, mpad, mrow, mside, mcorner, column, weights, lap1, lap2,
    load_sem, mass_send, mass_recv, edge_send, edge_recv,
):
    table = derivative_table()
    blocks_x, blocks_y = rows // 4, cols // 4
    pairs = cols // 2
    wide = -(-cols // SUB) * SUB
    face = lax.axis_index("face")
    col = lax.axis_index("col")
    up, down = lax.rem(face + faces - 1, faces), lax.rem(face + 1, faces)
    left, right = lax.rem(col + cols_axis - 1, cols_axis), lax.rem(col + 1, cols_axis)
    partners = (
        (up, col), (down, col), (face, left), (face, right),
        (up, left), (up, right), (down, left), (down, right),
    )

    barrier = pltpu.get_barrier_semaphore()
    for partner in partners:
        pl.semaphore_signal(barrier, inc=1, device_id=partner, device_id_type=MESH)

    small_loads = [
        pltpu.make_async_copy(source, target, load_sem.at[blocks_x + k])
        for k, (source, target) in enumerate(((diag, md), (cross, mc), (mass, mp)))
    ]

    def field_load(e):
        window = pl.ds(4 * e, 4)
        return pltpu.make_async_copy(fields.at[window], u.at[window], load_sem.at[e])

    for load in small_loads:
        load.start()
    for e in range(blocks_x):
        field_load(e).start()

    high = lax.broadcasted_iota(jnp.int32, (SUB, LANES), 0) >= SUB // 2

    def pair_tile(k, r, p):
        one = jnp.broadcast_to(column[k, r, pl.ds(2 * p, 1), :], (SUB, LANES))
        two = jnp.broadcast_to(column[k, r, pl.ds(2 * p + 1, 1), :], (SUB, LANES))
        weights[k, r, p] = jnp.where(high, two, one)

    def spread(k, turned):
        for r in range(rows):
            column[k, r] = jnp.broadcast_to(turned[:, r : r + 1], (wide, LANES))

        def pair_up(r, carry):
            for p in range(pairs):
                pair_tile(k, r, p)
            return carry

        lax.fori_loop(0, rows, pair_up, 0)

    def turned(value):
        square = lax.pad(value, np.float32(0), ((0, LANES - rows, 0), (0, LANES - cols, 0)))
        return jnp.transpose(square)[:wide]

    cid = lax.broadcasted_iota(jnp.int32, (wide, LANES), 0)
    rid = lax.broadcasted_iota(jnp.int32, (wide, LANES), 1)
    zero = jnp.zeros((wide, LANES), jnp.float32)
    valid = (rid < rows) & (cid < cols)

    def over_columns(centre):
        total = centre + jnp.where((cid % 4 == 0) & (cid > 0), pltpu.roll(centre, 1, 0), zero)
        return total + jnp.where((cid % 4 == 3) & (cid < cols - 1), pltpu.roll(centre, wide - 1, 0), zero)

    def over_rows(centre):
        total = centre + jnp.where((rid % 4 == 0) & (rid > 0), pltpu.roll(centre, 1, 1), zero)
        return total + jnp.where((rid % 4 == 3) & (rid < rows - 1), pltpu.roll(centre, LANES - 1, 1), zero)

    def inverse(total):
        return jnp.where(valid, 1.0 / jnp.where(valid, total, 1.0), 0.0)

    for load in small_loads:
        load.wait()
    mpad[...] = turned(mp[...])
    spread(0, turned(md[:, 0, :]))
    spread(1, turned(md[:, 1, :]))
    spread(2, turned(mc[...]))

    forward = pair_coefficients(table)
    backward = pair_coefficients(table.T)

    def laplace(values, e, g):
        grad_x = [combine(table, [values[a][q] for a in range(4)]) for q in range(2)]
        flux_x, flux_y = [[], []], []
        for a in range(4):
            grad_y = along(values[a], forward)
            line = []
            for q in range(2):
                first, second, mixed = (weights[k, 4 * e + a, 2 * g + q] for k in range(3))
                flux_x[q].append(first * grad_x[q][a] + mixed * grad_y[q])
                line.append(mixed * grad_x[q][a] + second * grad_y[q])
            flux_y.append(line)
        weak = [combine(table.T, flux_x[q]) for q in range(2)]
        for a in range(4):
            other = along(flux_y[a], backward)
            for q in range(2):
                weak[q][a] = weak[q][a] + other[q]
        return weak

    def keep(lap, e, g, weak):
        for a in range(4):
            for q in range(2):
                lap[4 * e + a + 1, 2 * g + q + 1] = weak[q][a]

    half = SUB // 2
    low_half, high_half = pl.ds(0, half), pl.ds(half, half)

    def remote(source, target, k, send_sem, recv_sem):
        return pltpu.make_async_remote_copy(
            src_ref=source,
            dst_ref=target,
            send_sem=send_sem,
            recv_sem=recv_sem,
            device_id=partners[k],
            device_id_type=MESH,
        )

    def edge_copies(phase, lap):
        inner, across = pl.ds(1, rows), pl.ds(1, pairs)
        moves = (
            (lap.at[1, across], lap.at[rows + 1, across]),
            (lap.at[rows, across], lap.at[0, across]),
            (lap.at[inner, 1, low_half], lap.at[inner, pairs + 1, low_half]),
            (lap.at[inner, pairs, high_half], lap.at[inner, 0, high_half]),
            (lap.at[1, 1, low_half], lap.at[rows + 1, pairs + 1, low_half]),
            (lap.at[1, pairs, high_half], lap.at[rows + 1, 0, high_half]),
            (lap.at[rows, 1, low_half], lap.at[0, pairs + 1, low_half]),
            (lap.at[rows, pairs, high_half], lap.at[0, 0, high_half]),
        )
        return [
            remote(source, target, k, edge_send.at[phase, k], edge_recv.at[phase, k])
            for k, (source, target) in enumerate(moves)
        ]

    def split_copies(lap):
        west_rows = (pl.ds(1, rows - 4), pl.ds(rows - 3, 4))
        east_rows = (pl.ds(5, rows - 4), pl.ds(1, 4))
        north_pairs = (pl.ds(1, pairs - 2), pl.ds(pairs - 1, 2))
        south_pairs = (pl.ds(3, pairs - 2), pl.ds(1, 2))
        pieces = []
        for n in range(2):
            line = (
                (lap.at[1, north_pairs[n]], lap.at[rows + 1, north_pairs[n]]),
                (lap.at[rows, south_pairs[n]], lap.at[0, south_pairs[n]]),
                (lap.at[west_rows[n], 1, low_half], lap.at[west_rows[n], pairs + 1, low_half]),
                (lap.at[east_rows[n], pairs, high_half], lap.at[east_rows[n], 0, high_half]),
            )
            pieces.append(
                [
                    remote(source, target, k, edge_send.at[1 + n, k], edge_recv.at[1 + n, k])
                    for k, (source, target) in enumerate(line)
                ]
            )
        return pieces

    left_tile, right_tile = mpad.at[pl.ds(0, SUB)], mpad.at[pl.ds(wide - SUB, SUB)]
    mass_moves = (
        (mpad, mside.at[1]), (mpad, mside.at[0]),
        (left_tile, mrow.at[1]), (right_tile, mrow.at[0]),
        (left_tile, mcorner.at[3]), (right_tile, mcorner.at[2]),
        (left_tile, mcorner.at[1]), (right_tile, mcorner.at[0]),
    )
    mass_copies = [
        remote(source, target, k, mass_send.at[k], mass_recv.at[k])
        for k, (source, target) in enumerate(mass_moves)
    ]

    def first_pass(e, carry):
        field_load(e).wait()
        for g in range(blocks_y):
            values = [[u[4 * e + a, 2 * g + q] for q in range(2)] for a in range(4)]
            keep(lap1, e, g, laplace(values, e, g))
        return carry

    lax.fori_loop(0, blocks_x, first_pass, 0)

    spread(3, inverse(over_rows(over_columns(mpad[...]))))

    pl.semaphore_wait(barrier, 8)
    first_copies = edge_copies(0, lap1)
    for copy in first_copies[4:] + mass_copies[4:] + mass_copies[2:4] + first_copies[2:4] + mass_copies[:2] + first_copies[:2]:
        copy.start()

    def assembled(lap, e, a, window):
        r = 4 * e + a

        def summed(p):
            part = lap[r + 1, p + 1]
            if a == 0:
                part = part + lap[r, p + 1]
            if a == 3:
                part = part + lap[r + 2, p + 1]
            return part

        parts = {}
        tiles = []
        for p in window:
            other = p - 1 if p % 2 == 0 else p + 1
            for q in (p, other):
                if q not in parts:
                    parts[q] = summed(q)
            turn = swap(parts[other])
            add = jnp.where(high, 0.0, turn) if p % 2 == 0 else jnp.where(high, turn, 0.0)
            tiles.append((parts[p] + add) * weights[3, r, p])
        return tiles

    def second(e, g):
        values = []
        for a in range(4):
            r = 4 * e + a
            parts = []
            for p in range(4):
                part = lap1[r + 1, 2 * g + p]
                if a == 0:
                    part = part + lap1[r, 2 * g + p]
                if a == 3:
                    part = part + lap1[r + 2, 2 * g + p]
                parts.append(part)
            left_tile = parts[1] + jnp.where(high, 0.0, swap(parts[0]))
            right_tile = parts[2] + jnp.where(high, swap(parts[3]), 0.0)
            values.append([left_tile * weights[3, r, 2 * g], right_tile * weights[3, r, 2 * g + 1]])
        keep(lap2, e, g, laplace(values, e, g))

    inner_blocks = range(1, blocks_y - 1)
    rim_blocks = (0, blocks_y - 1)

    def loop(low, high_end, body):
        def step(i, carry):
            body(i)
            return carry

        lax.fori_loop(low, high_end, step, 0)

    def over(blocks):
        def body(e):
            for g in blocks:
                second(e, g)

        return body

    inner_count = blocks_y - 2
    loop(0, (blocks_x - 2) * inner_count, lambda i: second(1 + i // inner_count, 1 + i % inner_count))

    def with_ends(centre, before, after):
        total = over_columns(centre)
        if before is not None:
            total = total + jnp.where(cid == 0, jnp.broadcast_to(before, (wide, LANES)), zero)
        if after is not None:
            total = total + jnp.where(cid == cols - 1, jnp.broadcast_to(after, (wide, LANES)), zero)
        return total

    def whole_inverse(west, east, north_west, north_east, south_west, south_east):
        north, south = with_ends(mside[0], north_west, north_east), with_ends(mside[1], south_west, south_east)
        total = over_rows(with_ends(mpad[...], west, east))
        total = total + jnp.where(rid == 0, pltpu.roll(north, LANES - rows + 1, 1), zero)
        return inverse(total + jnp.where(rid == rows - 1, pltpu.roll(south, rows - 1, 1), zero))

    def renew(full, r, p):
        start = 2 * p // SUB * SUB
        column[3, r, pl.ds(start, SUB), :] = jnp.broadcast_to(full[start : start + SUB, r : r + 1], (SUB, LANES))
        pair_tile(3, r, p)

    last = (cols - 1) % SUB
    def arrive(copies, which):
        for k in which:
            copies[k].wait_recv()

    second_copies = edge_copies(1, lap2)[4:]
    bulk, tip = split_copies(lap2)

    arrive(mass_copies, (0, 1))
    full = whole_inverse(None, None, None, None, None, None)
    for r in (0, rows - 1):
        column[3, r] = jnp.broadcast_to(full[:, r : r + 1], (wide, LANES))
        for p in range(pairs):
            pair_tile(3, r, p)
    arrive(first_copies, (0, 1))
    loop(0, 2 * inner_count, lambda i: second(i // inner_count * (blocks_x - 1), 1 + i % inner_count))

    arrive(mass_copies, (2, 4))
    from_east = (mrow[1, 0:1], mcorner[3, 0:1])
    full = whole_inverse(None, from_east[0], None, None, None, from_east[1])
    for r in range(rows):
        renew(full, r, pairs - 1)
    arrive(first_copies, (2, 4))
    second(blocks_x - 1, blocks_y - 1)
    second_copies[3].start()
    loop(1, blocks_x - 1, lambda e: second(e, blocks_y - 1))
    bulk[3].start()
    bulk[1].start()

    arrive(mass_copies, (3, 7))
    from_west = (mrow[0, last : last + 1], mcorner[0, last : last + 1])
    full = whole_inverse(from_west[0], from_east[0], from_west[1], None, None, from_east[1])
    for r in range(rows):
        renew(full, r, 0)
    arrive(first_copies, (3, 7))
    second(0, 0)
    second_copies[0].start()
    loop(1, blocks_x - 1, lambda e: second(e, 0))
    bulk[2].start()
    bulk[0].start()

    arrive(mass_copies, (5, 6))
    full = whole_inverse(
        from_west[0], from_east[0], from_west[1], mcorner[1, 0:1], mcorner[2, last : last + 1], from_east[1]
    )
    renew(full, 0, pairs - 1)
    renew(full, rows - 1, 0)
    arrive(first_copies, (5, 6))
    loop(0, 2, lambda i: second(i * (blocks_x - 1), (1 - i) * (blocks_y - 1)))
    for copy in second_copies[1:3] + tip[2:] + tip[:2]:
        copy.start()
    second_copies = second_copies + bulk + tip

    def write(e, a, window):
        for p, tile in zip(window, assembled(lap2, e, a, window)):
            out[4 * e + a, p] = tile

    middle, rim = tuple(range(1, pairs - 1)), (0, pairs - 1)

    def write_rows(window):
        for a in range(1, 4):
            write(0, a, window)
        for a in range(3):
            write(blocks_x - 1, a, window)

        def body(e):
            for a in range(4):
                write(e, a, window)

        loop(1, blocks_x - 1, body)

    write_rows(middle)
    for copy in second_copies:
        copy.wait_recv()
    write_rows(rim)
    write(0, 0, tuple(range(pairs)))
    write(blocks_x - 1, 3, tuple(range(pairs)))

    for copy in mass_copies + first_copies + second_copies:
        copy.wait_send()


def solution(mesh):
    faces, cols_axis = mesh.shape["face"], mesh.shape["col"]

    def shards(fields, metric_diag, metric_cross, point_mass):
        nfield, rows, cols, lanes = fields.shape
        wide = -(-cols // SUB) * SUB
        pairs = cols // 2
        f32 = jnp.float32
        anywhere = pl.BlockSpec(memory_space=pl.ANY)
        tiles = fields.transpose(1, 2, 0, 3).reshape(rows, pairs, 2 * nfield, lanes)
        result = pl.pallas_call(
            functools.partial(operator_kernel, faces, cols_axis, rows, cols),
            out_shape=pltpu.VMEM((rows, pairs, 2 * nfield, lanes), f32),
            in_specs=[anywhere] * 4,
            out_specs=pl.BlockSpec(memory_space=pltpu.VMEM),
            scratch_shapes=[
                pltpu.VMEM((rows, pairs, SUB, lanes), f32),
                pltpu.VMEM((rows, 2, cols), f32),
                pltpu.VMEM((rows, cols), f32),
                pltpu.VMEM((rows, cols), f32),
                pltpu.VMEM((wide, LANES), f32),
                pltpu.VMEM((2, SUB, LANES), f32),
                pltpu.VMEM((2, wide, LANES), f32),
                pltpu.VMEM((4, SUB, LANES), f32),
                pltpu.VMEM((4, rows, wide, LANES), f32),
                pltpu.VMEM((4, rows, pairs, SUB, LANES), f32),
                pltpu.VMEM((rows + 2, pairs + 2, SUB, lanes), f32),
                pltpu.VMEM((rows + 2, pairs + 2, SUB, lanes), f32),
                pltpu.SemaphoreType.DMA((rows // 4 + 3,)),
                pltpu.SemaphoreType.DMA((8,)),
                pltpu.SemaphoreType.DMA((8,)),
                pltpu.SemaphoreType.DMA((3, 8)),
                pltpu.SemaphoreType.DMA((3, 8)),
            ],
            compiler_params=pltpu.CompilerParams(collective_id=0, has_side_effects=True),
        )(tiles, metric_diag.transpose(1, 0, 2), metric_cross, point_mass)
        return result.reshape(rows, cols, nfield, lanes).transpose(2, 0, 1, 3)

    return jax.shard_map(
        shards,
        mesh=mesh,
        in_specs=(
            P(None, "face", "col", None),
            P(None, "face", "col"),
            P("face", "col"),
            P("face", "col"),
        ),
        out_specs=P(None, "face", "col", None),
        check_vma=False,
    )
```

```python
import functools

import jax
import jax.numpy as jnp
import numpy as np
from jax import lax
from jax.experimental import pallas as pl
from jax.experimental.pallas import tpu as pltpu
from jax.sharding import PartitionSpec as P

MESH = pl.DeviceIdType.MESH
SUB = 8
LANES = 128


def derivative_table():
    small = 1.0 / np.sqrt(5.0)
    nodes = np.array([-1.0, -small, small, 1.0])
    count = nodes.shape[0]
    weights = np.array(
        [np.prod([nodes[a] - nodes[k] for k in range(count) if k != a]) for a in range(count)]
    )
    table = np.zeros((count, count))
    for a in range(count):
        for b in range(count):
            if a == b:
                table[a, b] = np.sum([1.0 / (nodes[a] - nodes[k]) for k in range(count) if k != a])
            else:
                table[a, b] = weights[a] / weights[b] / (nodes[a] - nodes[b])
    table[np.abs(table) < 1e-12] = 0.0
    return table


def combine(table, parts):
    out = []
    for a in range(4):
        total = None
        for b in range(4):
            if table[a, b] == 0.0:
                continue
            term = np.float32(table[a, b]) * parts[b]
            total = term if total is None else total + term
        out.append(total)
    return out


def pair_coefficients(table):
    high = lax.broadcasted_iota(jnp.int32, (SUB, LANES), 0) >= SUB // 2
    result = []
    for p in range(2):
        line = []
        for q in range(2):
            kept = jnp.where(high, np.float32(table[2 * p + 1, 2 * q + 1]), np.float32(table[2 * p, 2 * q]))
            swapped = jnp.where(high, np.float32(table[2 * p + 1, 2 * q]), np.float32(table[2 * p, 2 * q + 1]))
            line.append((kept, swapped))
        result.append(line)
    return result


def swap(tile):
    return pltpu.roll(tile, SUB // 2, 0)


def along(pair, coefficients):
    turned = [swap(x) for x in pair]
    out = []
    for p in range(2):
        total = None
        for q in range(2):
            kept, swapped = coefficients[p][q]
            term = kept * pair[q] + swapped * turned[q]
            total = term if total is None else total + term
        out.append(total)
    return out


def operator_kernel(
    faces, cols_axis, rows, cols,
    fields, diag, cross, mass,
    out,
    u, md, mc, mp, mpad, mrow, mside, mcorner, column, weights, lap1, lap2,
    load_sem, mass_send, mass_recv, edge_send, edge_recv,
):
    table = derivative_table()
    blocks_x, blocks_y = rows // 4, cols // 4
    pairs = cols // 2
    wide = -(-cols // SUB) * SUB
    face = lax.axis_index("face")
    col = lax.axis_index("col")
    up, down = lax.rem(face + faces - 1, faces), lax.rem(face + 1, faces)
    left, right = lax.rem(col + cols_axis - 1, cols_axis), lax.rem(col + 1, cols_axis)
    partners = (
        (up, col), (down, col), (face, left), (face, right),
        (up, left), (up, right), (down, left), (down, right),
    )

    barrier = pltpu.get_barrier_semaphore()
    for partner in partners:
        pl.semaphore_signal(barrier, inc=1, device_id=partner, device_id_type=MESH)

    small_loads = [
        pltpu.make_async_copy(source, target, load_sem.at[blocks_x + k])
        for k, (source, target) in enumerate(((diag, md), (cross, mc), (mass, mp)))
    ]

    def field_load(e):
        window = pl.ds(4 * e, 4)
        return pltpu.make_async_copy(fields.at[window], u.at[window], load_sem.at[e])

    for load in small_loads:
        load.start()
    for e in range(blocks_x):
        field_load(e).start()

    high = lax.broadcasted_iota(jnp.int32, (SUB, LANES), 0) >= SUB // 2

    def pair_tile(k, r, p):
        one = jnp.broadcast_to(column[k, r, pl.ds(2 * p, 1), :], (SUB, LANES))
        two = jnp.broadcast_to(column[k, r, pl.ds(2 * p + 1, 1), :], (SUB, LANES))
        weights[k, r, p] = jnp.where(high, two, one)

    def spread(k, turned):
        for r in range(rows):
            column[k, r] = jnp.broadcast_to(turned[:, r : r + 1], (wide, LANES))

        def pair_up(r, carry):
            for p in range(pairs):
                pair_tile(k, r, p)
            return carry

        lax.fori_loop(0, rows, pair_up, 0)

    def turned(value):
        square = lax.pad(value, np.float32(0), ((0, LANES - rows, 0), (0, LANES - cols, 0)))
        return jnp.transpose(square)[:wide]

    cid = lax.broadcasted_iota(jnp.int32, (wide, LANES), 0)
    rid = lax.broadcasted_iota(jnp.int32, (wide, LANES), 1)
    zero = jnp.zeros((wide, LANES), jnp.float32)
    valid = (rid < rows) & (cid < cols)

    def over_columns(centre):
        total = centre + jnp.where((cid % 4 == 0) & (cid > 0), pltpu.roll(centre, 1, 0), zero)
        return total + jnp.where((cid % 4 == 3) & (cid < cols - 1), pltpu.roll(centre, wide - 1, 0), zero)

    def over_rows(centre):
        total = centre + jnp.where((rid % 4 == 0) & (rid > 0), pltpu.roll(centre, 1, 1), zero)
        return total + jnp.where((rid % 4 == 3) & (rid < rows - 1), pltpu.roll(centre, LANES - 1, 1), zero)

    def inverse(total):
        return jnp.where(valid, 1.0 / jnp.where(valid, total, 1.0), 0.0)

    for load in small_loads:
        load.wait()
    mpad[...] = turned(mp[...])
    spread(0, turned(md[:, 0, :]))
    spread(1, turned(md[:, 1, :]))
    spread(2, turned(mc[...]))

    forward = pair_coefficients(table)
    backward = pair_coefficients(table.T)

    def laplace(values, e, g):
        grad_x = [combine(table, [values[a][q] for a in range(4)]) for q in range(2)]
        flux_x, flux_y = [[], []], []
        for a in range(4):
            grad_y = along(values[a], forward)
            line = []
            for q in range(2):
                first, second, mixed = (weights[k, 4 * e + a, 2 * g + q] for k in range(3))
                flux_x[q].append(first * grad_x[q][a] + mixed * grad_y[q])
                line.append(mixed * grad_x[q][a] + second * grad_y[q])
            flux_y.append(line)
        weak = [combine(table.T, flux_x[q]) for q in range(2)]
        for a in range(4):
            other = along(flux_y[a], backward)
            for q in range(2):
                weak[q][a] = weak[q][a] + other[q]
        return weak

    def keep(lap, e, g, weak):
        for a in range(4):
            for q in range(2):
                lap[4 * e + a + 1, 2 * g + q + 1] = weak[q][a]

    half = SUB // 2
    low_half, high_half = pl.ds(0, half), pl.ds(half, half)

    def remote(source, target, k, send_sem, recv_sem):
        return pltpu.make_async_remote_copy(
            src_ref=source,
            dst_ref=target,
            send_sem=send_sem,
            recv_sem=recv_sem,
            device_id=partners[k],
            device_id_type=MESH,
        )

    def edge_copies(phase, lap):
        inner, across = pl.ds(1, rows), pl.ds(1, pairs)
        moves = (
            (lap.at[1, across], lap.at[rows + 1, across]),
            (lap.at[rows, across], lap.at[0, across]),
            (lap.at[inner, 1, low_half], lap.at[inner, pairs + 1, low_half]),
            (lap.at[inner, pairs, high_half], lap.at[inner, 0, high_half]),
            (lap.at[1, 1, low_half], lap.at[rows + 1, pairs + 1, low_half]),
            (lap.at[1, pairs, high_half], lap.at[rows + 1, 0, high_half]),
            (lap.at[rows, 1, low_half], lap.at[0, pairs + 1, low_half]),
            (lap.at[rows, pairs, high_half], lap.at[0, 0, high_half]),
        )
        return [
            remote(source, target, k, edge_send.at[phase, k], edge_recv.at[phase, k])
            for k, (source, target) in enumerate(moves)
        ]

    def split_copies(lap):
        west_rows = (pl.ds(1, rows - 4), pl.ds(rows - 3, 4))
        east_rows = (pl.ds(5, rows - 4), pl.ds(1, 4))
        north_pairs = (pl.ds(1, pairs - 2), pl.ds(pairs - 1, 2))
        south_pairs = (pl.ds(3, pairs - 2), pl.ds(1, 2))
        pieces = []
        for n in range(2):
            line = (
                (lap.at[1, north_pairs[n]], lap.at[rows + 1, north_pairs[n]]),
                (lap.at[rows, south_pairs[n]], lap.at[0, south_pairs[n]]),
                (lap.at[west_rows[n], 1, low_half], lap.at[west_rows[n], pairs + 1, low_half]),
                (lap.at[east_rows[n], pairs, high_half], lap.at[east_rows[n], 0, high_half]),
            )
            pieces.append(
                [
                    remote(source, target, k, edge_send.at[1 + n, k], edge_recv.at[1 + n, k])
                    for k, (source, target) in enumerate(line)
                ]
            )
        return pieces

    left_tile, right_tile = mpad.at[pl.ds(0, SUB)], mpad.at[pl.ds(wide - SUB, SUB)]
    mass_moves = (
        (mpad, mside.at[1]), (mpad, mside.at[0]),
        (left_tile, mrow.at[1]), (right_tile, mrow.at[0]),
        (left_tile, mcorner.at[3]), (right_tile, mcorner.at[2]),
        (left_tile, mcorner.at[1]), (right_tile, mcorner.at[0]),
    )
    mass_copies = [
        remote(source, target, k, mass_send.at[k], mass_recv.at[k])
        for k, (source, target) in enumerate(mass_moves)
    ]

    def first_pass(e, carry):
        field_load(e).wait()
        for g in range(blocks_y):
            values = [[u[4 * e + a, 2 * g + q] for q in range(2)] for a in range(4)]
            keep(lap1, e, g, laplace(values, e, g))
        return carry

    lax.fori_loop(0, blocks_x, first_pass, 0)

    spread(3, inverse(over_rows(over_columns(mpad[...]))))

    pl.semaphore_wait(barrier, 8)
    first_copies = edge_copies(0, lap1)
    for copy in first_copies[4:] + mass_copies[4:] + mass_copies[2:4] + first_copies[2:4] + mass_copies[:2] + first_copies[:2]:
        copy.start()

    def assembled(lap, e, a, window):
        r = 4 * e + a

        def summed(p):
            part = lap[r + 1, p + 1]
            if a == 0:
                part = part + lap[r, p + 1]
            if a == 3:
                part = part + lap[r + 2, p + 1]
            return part

        parts = {}
        tiles = []
        for p in window:
            other = p - 1 if p % 2 == 0 else p + 1
            for q in (p, other):
                if q not in parts:
                    parts[q] = summed(q)
            turn = swap(parts[other])
            add = jnp.where(high, 0.0, turn) if p % 2 == 0 else jnp.where(high, turn, 0.0)
            tiles.append((parts[p] + add) * weights[3, r, p])
        return tiles

    def second(e, g):
        values = []
        for a in range(4):
            r = 4 * e + a
            parts = []
            for p in range(4):
                part = lap1[r + 1, 2 * g + p]
                if a == 0:
                    part = part + lap1[r, 2 * g + p]
                if a == 3:
                    part = part + lap1[r + 2, 2 * g + p]
                parts.append(part)
            left_tile = parts[1] + jnp.where(high, 0.0, swap(parts[0]))
            right_tile = parts[2] + jnp.where(high, swap(parts[3]), 0.0)
            values.append([left_tile * weights[3, r, 2 * g], right_tile * weights[3, r, 2 * g + 1]])
        keep(lap2, e, g, laplace(values, e, g))

    inner_blocks = range(1, blocks_y - 1)
    rim_blocks = (0, blocks_y - 1)

    def loop(low, high_end, body):
        def step(i, carry):
            body(i)
            return carry

        lax.fori_loop(low, high_end, step, 0)

    def over(blocks):
        def body(e):
            for g in blocks:
                second(e, g)

        return body

    inner_count = blocks_y - 2
    loop(0, (blocks_x - 2) * inner_count, lambda i: second(1 + i // inner_count, 1 + i % inner_count))

    def with_ends(centre, before, after):
        total = over_columns(centre)
        if before is not None:
            total = total + jnp.where(cid == 0, jnp.broadcast_to(before, (wide, LANES)), zero)
        if after is not None:
            total = total + jnp.where(cid == cols - 1, jnp.broadcast_to(after, (wide, LANES)), zero)
        return total

    def whole_inverse(west, east, north_west, north_east, south_west, south_east):
        north, south = with_ends(mside[0], north_west, north_east), with_ends(mside[1], south_west, south_east)
        total = over_rows(with_ends(mpad[...], west, east))
        total = total + jnp.where(rid == 0, pltpu.roll(north, LANES - rows + 1, 1), zero)
        return inverse(total + jnp.where(rid == rows - 1, pltpu.roll(south, rows - 1, 1), zero))

    def renew(full, r, p):
        start = 2 * p // SUB * SUB
        column[3, r, pl.ds(start, SUB), :] = jnp.broadcast_to(full[start : start + SUB, r : r + 1], (SUB, LANES))
        pair_tile(3, r, p)

    last = (cols - 1) % SUB
    def arrive(copies, which):
        for k in which:
            copies[k].wait_recv()

    second_copies = edge_copies(1, lap2)[4:]
    bulk, tip = split_copies(lap2)

    arrive(mass_copies, (0, 1))
    full = whole_inverse(None, None, None, None, None, None)
    for r in (0, rows - 1):
        column[3, r] = jnp.broadcast_to(full[:, r : r + 1], (wide, LANES))
        for p in range(pairs):
            pair_tile(3, r, p)
    arrive(first_copies, (0, 1))
    loop(0, 2 * inner_count, lambda i: second(i // inner_count * (blocks_x - 1), 1 + i % inner_count))

    arrive(mass_copies, (2, 4))
    from_east = (mrow[1, 0:1], mcorner[3, 0:1])
    full = whole_inverse(None, from_east[0], None, None, None, from_east[1])
    for r in range(rows):
        renew(full, r, pairs - 1)
    arrive(first_copies, (2, 4))
    second(blocks_x - 1, blocks_y - 1)
    second_copies[3].start()
    loop(1, blocks_x - 1, lambda e: second(e, blocks_y - 1))
    bulk[3].start()
    bulk[1].start()

    arrive(mass_copies, (3, 7))
    from_west = (mrow[0, last : last + 1], mcorner[0, last : last + 1])
    full = whole_inverse(from_west[0], from_east[0], from_west[1], None, None, from_east[1])
    for r in range(rows):
        renew(full, r, 0)
    arrive(first_copies, (3, 7))
    second(0, 0)
    second_copies[0].start()
    loop(1, blocks_x - 1, lambda e: second(e, 0))
    bulk[2].start()
    bulk[0].start()

    arrive(mass_copies, (5, 6))
    full = whole_inverse(
        from_west[0], from_east[0], from_west[1], mcorner[1, 0:1], mcorner[2, last : last + 1], from_east[1]
    )
    renew(full, 0, pairs - 1)
    renew(full, rows - 1, 0)
    arrive(first_copies, (5, 6))
    loop(0, 2, lambda i: second(i * (blocks_x - 1), (1 - i) * (blocks_y - 1)))
    for copy in second_copies[1:3] + tip[2:] + tip[:2]:
        copy.start()
    second_copies = second_copies + bulk + tip

    def write(e, a, window):
        for p, tile in zip(window, assembled(lap2, e, a, window)):
            out[4 * e + a, p] = tile

    middle = tuple(range(1, pairs - 1))

    def write_rows(window):
        for a in range(1, 4):
            write(0, a, window)
        for a in range(3):
            write(blocks_x - 1, a, window)

        def body(e):
            for a in range(4):
                write(e, a, window)

        loop(1, blocks_x - 1, body)

    write_rows(middle)
    for copy in bulk[:2] + tip[:2]:
        copy.wait_recv()
    write(0, 0, middle)
    write(blocks_x - 1, 3, middle)

    def write_side(p):
        def body(e):
            for a in range(4):
                write(e, a, (p,))

        loop(0, blocks_x, body)

    for copy in (bulk[2], tip[2], second_copies[0], second_copies[2]):
        copy.wait_recv()
    write_side(pairs - 1)
    for copy in (bulk[3], tip[3], second_copies[1], second_copies[3]):
        copy.wait_recv()
    write_side(0)

    for copy in mass_copies + first_copies + second_copies:
        copy.wait_send()


def solution(mesh):
    faces, cols_axis = mesh.shape["face"], mesh.shape["col"]

    def shards(fields, metric_diag, metric_cross, point_mass):
        nfield, rows, cols, lanes = fields.shape
        wide = -(-cols // SUB) * SUB
        pairs = cols // 2
        f32 = jnp.float32
        anywhere = pl.BlockSpec(memory_space=pl.ANY)
        tiles = fields.transpose(1, 2, 0, 3).reshape(rows, pairs, 2 * nfield, lanes)
        result = pl.pallas_call(
            functools.partial(operator_kernel, faces, cols_axis, rows, cols),
            out_shape=pltpu.VMEM((rows, pairs, 2 * nfield, lanes), f32),
            in_specs=[anywhere] * 4,
            out_specs=pl.BlockSpec(memory_space=pltpu.VMEM),
            scratch_shapes=[
                pltpu.VMEM((rows, pairs, SUB, lanes), f32),
                pltpu.VMEM((rows, 2, cols), f32),
                pltpu.VMEM((rows, cols), f32),
                pltpu.VMEM((rows, cols), f32),
                pltpu.VMEM((wide, LANES), f32),
                pltpu.VMEM((2, SUB, LANES), f32),
                pltpu.VMEM((2, wide, LANES), f32),
                pltpu.VMEM((4, SUB, LANES), f32),
                pltpu.VMEM((4, rows, wide, LANES), f32),
                pltpu.VMEM((4, rows, pairs, SUB, LANES), f32),
                pltpu.VMEM((rows + 2, pairs + 2, SUB, lanes), f32),
                pltpu.VMEM((rows + 2, pairs + 2, SUB, lanes), f32),
                pltpu.SemaphoreType.DMA((rows // 4 + 3,)),
                pltpu.SemaphoreType.DMA((8,)),
                pltpu.SemaphoreType.DMA((8,)),
                pltpu.SemaphoreType.DMA((3, 8)),
                pltpu.SemaphoreType.DMA((3, 8)),
            ],
            compiler_params=pltpu.CompilerParams(collective_id=0, has_side_effects=True),
        )(tiles, metric_diag.transpose(1, 0, 2), metric_cross, point_mass)
        return result.reshape(rows, cols, nfield, lanes).transpose(2, 0, 1, 3)

    return jax.shard_map(
        shards,
        mesh=mesh,
        in_specs=(
            P(None, "face", "col", None),
            P(None, "face", "col"),
            P("face", "col"),
            P("face", "col"),
        ),
        out_specs=P(None, "face", "col", None),
        check_vma=False,
    )
```

```python
import functools

import jax
import jax.numpy as jnp
import numpy as np
from jax import lax
from jax.experimental import pallas as pl
from jax.experimental.pallas import tpu as pltpu
from jax.sharding import PartitionSpec as P

MESH = pl.DeviceIdType.MESH
SUB = 8
LANES = 128


def derivative_table():
    small = 1.0 / np.sqrt(5.0)
    nodes = np.array([-1.0, -small, small, 1.0])
    count = nodes.shape[0]
    weights = np.array(
        [np.prod([nodes[a] - nodes[k] for k in range(count) if k != a]) for a in range(count)]
    )
    table = np.zeros((count, count))
    for a in range(count):
        for b in range(count):
            if a == b:
                table[a, b] = np.sum([1.0 / (nodes[a] - nodes[k]) for k in range(count) if k != a])
            else:
                table[a, b] = weights[a] / weights[b] / (nodes[a] - nodes[b])
    table[np.abs(table) < 1e-12] = 0.0
    return table


def combine(table, parts):
    out = []
    for a in range(4):
        total = None
        for b in range(4):
            if table[a, b] == 0.0:
                continue
            term = np.float32(table[a, b]) * parts[b]
            total = term if total is None else total + term
        out.append(total)
    return out


def pair_coefficients(table):
    high = lax.broadcasted_iota(jnp.int32, (SUB, LANES), 0) >= SUB // 2
    result = []
    for p in range(2):
        line = []
        for q in range(2):
            kept = jnp.where(high, np.float32(table[2 * p + 1, 2 * q + 1]), np.float32(table[2 * p, 2 * q]))
            swapped = jnp.where(high, np.float32(table[2 * p + 1, 2 * q]), np.float32(table[2 * p, 2 * q + 1]))
            line.append((kept, swapped))
        result.append(line)
    return result


def swap(tile):
    return pltpu.roll(tile, SUB // 2, 0)


def along(pair, coefficients):
    turned = [swap(x) for x in pair]
    out = []
    for p in range(2):
        total = None
        for q in range(2):
            kept, swapped = coefficients[p][q]
            term = kept * pair[q] + swapped * turned[q]
            total = term if total is None else total + term
        out.append(total)
    return out


def operator_kernel(
    faces, cols_axis, rows, cols,
    fields, diag, cross, mass,
    out,
    u, md, mc, mp, mpad, mrow, mside, mcorner, column, weights, lap1, lap2,
    load_sem, mass_send, mass_recv, edge_send, edge_recv,
):
    table = derivative_table()
    blocks_x, blocks_y = rows // 4, cols // 4
    pairs = cols // 2
    wide = -(-cols // SUB) * SUB
    face = lax.axis_index("face")
    col = lax.axis_index("col")
    up, down = lax.rem(face + faces - 1, faces), lax.rem(face + 1, faces)
    left, right = lax.rem(col + cols_axis - 1, cols_axis), lax.rem(col + 1, cols_axis)
    partners = (
        (up, col), (down, col), (face, left), (face, right),
        (up, left), (up, right), (down, left), (down, right),
    )

    barrier = pltpu.get_barrier_semaphore()
    for partner in partners:
        pl.semaphore_signal(barrier, inc=1, device_id=partner, device_id_type=MESH)

    small_loads = [
        pltpu.make_async_copy(source, target, load_sem.at[blocks_x + k])
        for k, (source, target) in enumerate(((diag, md), (cross, mc), (mass, mp)))
    ]

    def field_load(e):
        window = pl.ds(4 * e, 4)
        return pltpu.make_async_copy(fields.at[window], u.at[window], load_sem.at[e])

    for load in small_loads:
        load.start()
    for e in range(blocks_x):
        field_load(e).start()

    high = lax.broadcasted_iota(jnp.int32, (SUB, LANES), 0) >= SUB // 2

    def pair_tile(k, r, p):
        one = jnp.broadcast_to(column[k, r, pl.ds(2 * p, 1), :], (SUB, LANES))
        two = jnp.broadcast_to(column[k, r, pl.ds(2 * p + 1, 1), :], (SUB, LANES))
        weights[k, r, p] = jnp.where(high, two, one)

    def spread(k, turned):
        for r in range(rows):
            column[k, r] = jnp.broadcast_to(turned[:, r : r + 1], (wide, LANES))

        def pair_up(r, carry):
            for p in range(pairs):
                pair_tile(k, r, p)
            return carry

        lax.fori_loop(0, rows, pair_up, 0)

    def turned(value):
        square = lax.pad(value, np.float32(0), ((0, LANES - rows, 0), (0, LANES - cols, 0)))
        return jnp.transpose(square)[:wide]

    cid = lax.broadcasted_iota(jnp.int32, (wide, LANES), 0)
    rid = lax.broadcasted_iota(jnp.int32, (wide, LANES), 1)
    zero = jnp.zeros((wide, LANES), jnp.float32)
    valid = (rid < rows) & (cid < cols)

    def over_columns(centre):
        total = centre + jnp.where((cid % 4 == 0) & (cid > 0), pltpu.roll(centre, 1, 0), zero)
        return total + jnp.where((cid % 4 == 3) & (cid < cols - 1), pltpu.roll(centre, wide - 1, 0), zero)

    def over_rows(centre):
        total = centre + jnp.where((rid % 4 == 0) & (rid > 0), pltpu.roll(centre, 1, 1), zero)
        return total + jnp.where((rid % 4 == 3) & (rid < rows - 1), pltpu.roll(centre, LANES - 1, 1), zero)

    def inverse(total):
        return jnp.where(valid, 1.0 / jnp.where(valid, total, 1.0), 0.0)

    for load in small_loads:
        load.wait()
    mpad[...] = turned(mp[...])
    spread(0, turned(md[:, 0, :]))
    spread(1, turned(md[:, 1, :]))
    spread(2, turned(mc[...]))

    forward = pair_coefficients(table)
    backward = pair_coefficients(table.T)

    def laplace(values, e, g):
        grad_x = [combine(table, [values[a][q] for a in range(4)]) for q in range(2)]
        flux_x, flux_y = [[], []], []
        for a in range(4):
            grad_y = along(values[a], forward)
            line = []
            for q in range(2):
                first, second, mixed = (weights[k, 4 * e + a, 2 * g + q] for k in range(3))
                flux_x[q].append(first * grad_x[q][a] + mixed * grad_y[q])
                line.append(mixed * grad_x[q][a] + second * grad_y[q])
            flux_y.append(line)
        weak = [combine(table.T, flux_x[q]) for q in range(2)]
        for a in range(4):
            other = along(flux_y[a], backward)
            for q in range(2):
                weak[q][a] = weak[q][a] + other[q]
        return weak

    def keep(lap, e, g, weak):
        for a in range(4):
            for q in range(2):
                lap[4 * e + a + 1, 2 * g + q + 1] = weak[q][a]

    half = SUB // 2
    low_half, high_half = pl.ds(0, half), pl.ds(half, half)

    def remote(source, target, k, send_sem, recv_sem):
        return pltpu.make_async_remote_copy(
            src_ref=source,
            dst_ref=target,
            send_sem=send_sem,
            recv_sem=recv_sem,
            device_id=partners[k],
            device_id_type=MESH,
        )

    def edge_copies(phase, lap):
        inner, across = pl.ds(1, rows), pl.ds(1, pairs)
        moves = (
            (lap.at[1, across], lap.at[rows + 1, across]),
            (lap.at[rows, across], lap.at[0, across]),
            (lap.at[inner, 1, low_half], lap.at[inner, pairs + 1, low_half]),
            (lap.at[inner, pairs, high_half], lap.at[inner, 0, high_half]),
            (lap.at[1, 1, low_half], lap.at[rows + 1, pairs + 1, low_half]),
            (lap.at[1, pairs, high_half], lap.at[rows + 1, 0, high_half]),
            (lap.at[rows, 1, low_half], lap.at[0, pairs + 1, low_half]),
            (lap.at[rows, pairs, high_half], lap.at[0, 0, high_half]),
        )
        return [
            remote(source, target, k, edge_send.at[phase, k], edge_recv.at[phase, k])
            for k, (source, target) in enumerate(moves)
        ]

    def split_copies(lap):
        west_rows = (pl.ds(1, rows - 4), pl.ds(rows - 3, 4))
        east_rows = (pl.ds(5, rows - 4), pl.ds(1, 4))
        north_pairs = (pl.ds(1, pairs - 2), pl.ds(pairs - 1, 2))
        south_pairs = (pl.ds(3, pairs - 2), pl.ds(1, 2))
        pieces = []
        for n in range(2):
            line = (
                (lap.at[1, north_pairs[n]], lap.at[rows + 1, north_pairs[n]]),
                (lap.at[rows, south_pairs[n]], lap.at[0, south_pairs[n]]),
                (lap.at[west_rows[n], 1, low_half], lap.at[west_rows[n], pairs + 1, low_half]),
                (lap.at[east_rows[n], pairs, high_half], lap.at[east_rows[n], 0, high_half]),
            )
            pieces.append(
                [
                    remote(source, target, k, edge_send.at[1 + n, k], edge_recv.at[1 + n, k])
                    for k, (source, target) in enumerate(line)
                ]
            )
        return pieces

    left_tile, right_tile = mpad.at[low_half], mpad.at[pl.ds(wide - SUB, half)]
    mass_moves = (
        (mpad, mside.at[1]), (mpad, mside.at[0]),
        (left_tile, mrow.at[1, low_half]), (right_tile, mrow.at[0, low_half]),
        (left_tile, mcorner.at[3, low_half]), (right_tile, mcorner.at[2, low_half]),
        (left_tile, mcorner.at[1, low_half]), (right_tile, mcorner.at[0, low_half]),
    )
    mass_copies = [
        remote(source, target, k, mass_send.at[k], mass_recv.at[k])
        for k, (source, target) in enumerate(mass_moves)
    ]

    def first_pass(e, carry):
        field_load(e).wait()
        for g in range(blocks_y):
            values = [[u[4 * e + a, 2 * g + q] for q in range(2)] for a in range(4)]
            keep(lap1, e, g, laplace(values, e, g))
        return carry

    lax.fori_loop(0, blocks_x, first_pass, 0)

    spread(3, inverse(over_rows(over_columns(mpad[...]))))

    pl.semaphore_wait(barrier, 8)
    first_copies = edge_copies(0, lap1)
    for copy in first_copies[4:] + mass_copies[4:] + mass_copies[2:4] + first_copies[2:4] + mass_copies[:2] + first_copies[:2]:
        copy.start()

    def assembled(lap, e, a, window):
        r = 4 * e + a

        def summed(p):
            part = lap[r + 1, p + 1]
            if a == 0:
                part = part + lap[r, p + 1]
            if a == 3:
                part = part + lap[r + 2, p + 1]
            return part

        parts = {}
        tiles = []
        for p in window:
            other = p - 1 if p % 2 == 0 else p + 1
            for q in (p, other):
                if q not in parts:
                    parts[q] = summed(q)
            turn = swap(parts[other])
            add = jnp.where(high, 0.0, turn) if p % 2 == 0 else jnp.where(high, turn, 0.0)
            tiles.append((parts[p] + add) * weights[3, r, p])
        return tiles

    def second(e, g):
        values = []
        for a in range(4):
            r = 4 * e + a
            parts = []
            for p in range(4):
                part = lap1[r + 1, 2 * g + p]
                if a == 0:
                    part = part + lap1[r, 2 * g + p]
                if a == 3:
                    part = part + lap1[r + 2, 2 * g + p]
                parts.append(part)
            left_tile = parts[1] + jnp.where(high, 0.0, swap(parts[0]))
            right_tile = parts[2] + jnp.where(high, swap(parts[3]), 0.0)
            values.append([left_tile * weights[3, r, 2 * g], right_tile * weights[3, r, 2 * g + 1]])
        keep(lap2, e, g, laplace(values, e, g))

    inner_blocks = range(1, blocks_y - 1)
    rim_blocks = (0, blocks_y - 1)

    def loop(low, high_end, body):
        def step(i, carry):
            body(i)
            return carry

        lax.fori_loop(low, high_end, step, 0)

    def over(blocks):
        def body(e):
            for g in blocks:
                second(e, g)

        return body

    inner_count = blocks_y - 2
    loop(0, (blocks_x - 2) * inner_count, lambda i: second(1 + i // inner_count, 1 + i % inner_count))

    def with_ends(centre, before, after):
        total = over_columns(centre)
        if before is not None:
            total = total + jnp.where(cid == 0, jnp.broadcast_to(before, (wide, LANES)), zero)
        if after is not None:
            total = total + jnp.where(cid == cols - 1, jnp.broadcast_to(after, (wide, LANES)), zero)
        return total

    def whole_inverse(west, east, north_west, north_east, south_west, south_east):
        north, south = with_ends(mside[0], north_west, north_east), with_ends(mside[1], south_west, south_east)
        total = over_rows(with_ends(mpad[...], west, east))
        total = total + jnp.where(rid == 0, pltpu.roll(north, LANES - rows + 1, 1), zero)
        return inverse(total + jnp.where(rid == rows - 1, pltpu.roll(south, rows - 1, 1), zero))

    def renew(full, r, p):
        start = 2 * p // SUB * SUB
        column[3, r, pl.ds(start, SUB), :] = jnp.broadcast_to(full[start : start + SUB, r : r + 1], (SUB, LANES))
        pair_tile(3, r, p)

    last = (cols - 1) % SUB
    def arrive(copies, which):
        for k in which:
            copies[k].wait_recv()

    second_copies = edge_copies(1, lap2)[4:]
    bulk, tip = split_copies(lap2)

    arrive(mass_copies, (0, 1))
    full = whole_inverse(None, None, None, None, None, None)
    for r in (0, rows - 1):
        column[3, r] = jnp.broadcast_to(full[:, r : r + 1], (wide, LANES))
        for p in range(pairs):
            pair_tile(3, r, p)
    arrive(first_copies, (0, 1))
    loop(0, 2 * inner_count, lambda i: second(i // inner_count * (blocks_x - 1), 1 + i % inner_count))

    arrive(mass_copies, (2, 4))
    from_east = (mrow[1, 0:1], mcorner[3, 0:1])
    full = whole_inverse(None, from_east[0], None, None, None, from_east[1])
    for r in range(rows):
        renew(full, r, pairs - 1)
    arrive(first_copies, (2, 4))
    second(blocks_x - 1, blocks_y - 1)
    second_copies[3].start()
    loop(1, blocks_x - 1, lambda e: second(e, blocks_y - 1))
    bulk[3].start()
    bulk[1].start()

    arrive(mass_copies, (3, 7))
    from_west = (mrow[0, last : last + 1], mcorner[0, last : last + 1])
    full = whole_inverse(from_west[0], from_east[0], from_west[1], None, None, from_east[1])
    for r in range(rows):
        renew(full, r, 0)
    arrive(first_copies, (3, 7))
    second(0, 0)
    second_copies[0].start()
    loop(1, blocks_x - 1, lambda e: second(e, 0))
    bulk[2].start()
    bulk[0].start()

    arrive(mass_copies, (5, 6))
    full = whole_inverse(
        from_west[0], from_east[0], from_west[1], mcorner[1, 0:1], mcorner[2, last : last + 1], from_east[1]
    )
    renew(full, 0, pairs - 1)
    renew(full, rows - 1, 0)
    arrive(first_copies, (5, 6))
    loop(0, 2, lambda i: second(i * (blocks_x - 1), (1 - i) * (blocks_y - 1)))
    for copy in second_copies[1:3] + tip[2:] + tip[:2]:
        copy.start()
    second_copies = second_copies + bulk + tip

    def write(e, a, window):
        for p, tile in zip(window, assembled(lap2, e, a, window)):
            out[4 * e + a, p] = tile

    middle = tuple(range(1, pairs - 1))

    def write_rows(window):
        for a in range(1, 4):
            write(0, a, window)
        for a in range(3):
            write(blocks_x - 1, a, window)

        def body(e):
            for a in range(4):
                write(e, a, window)

        loop(1, blocks_x - 1, body)

    write_rows(middle)
    for copy in bulk[:2] + tip[:2]:
        copy.wait_recv()
    write(0, 0, middle)
    write(blocks_x - 1, 3, middle)

    def write_side(p):
        def body(e):
            for a in range(4):
                write(e, a, (p,))

        loop(0, blocks_x, body)

    for copy in (bulk[2], tip[2], second_copies[0], second_copies[2]):
        copy.wait_recv()
    write_side(pairs - 1)
    for copy in (bulk[3], tip[3], second_copies[1], second_copies[3]):
        copy.wait_recv()
    write_side(0)

    for copy in mass_copies + first_copies + second_copies:
        copy.wait_send()


def solution(mesh):
    faces, cols_axis = mesh.shape["face"], mesh.shape["col"]

    def shards(fields, metric_diag, metric_cross, point_mass):
        nfield, rows, cols, lanes = fields.shape
        wide = -(-cols // SUB) * SUB
        pairs = cols // 2
        f32 = jnp.float32
        anywhere = pl.BlockSpec(memory_space=pl.ANY)
        tiles = fields.transpose(1, 2, 0, 3).reshape(rows, pairs, 2 * nfield, lanes)
        result = pl.pallas_call(
            functools.partial(operator_kernel, faces, cols_axis, rows, cols),
            out_shape=pltpu.VMEM((rows, pairs, 2 * nfield, lanes), f32),
            in_specs=[anywhere] * 4,
            out_specs=pl.BlockSpec(memory_space=pltpu.VMEM),
            scratch_shapes=[
                pltpu.VMEM((rows, pairs, SUB, lanes), f32),
                pltpu.VMEM((rows, 2, cols), f32),
                pltpu.VMEM((rows, cols), f32),
                pltpu.VMEM((rows, cols), f32),
                pltpu.VMEM((wide, LANES), f32),
                pltpu.VMEM((2, SUB, LANES), f32),
                pltpu.VMEM((2, wide, LANES), f32),
                pltpu.VMEM((4, SUB, LANES), f32),
                pltpu.VMEM((4, rows, wide, LANES), f32),
                pltpu.VMEM((4, rows, pairs, SUB, LANES), f32),
                pltpu.VMEM((rows + 2, pairs + 2, SUB, lanes), f32),
                pltpu.VMEM((rows + 2, pairs + 2, SUB, lanes), f32),
                pltpu.SemaphoreType.DMA((rows // 4 + 3,)),
                pltpu.SemaphoreType.DMA((8,)),
                pltpu.SemaphoreType.DMA((8,)),
                pltpu.SemaphoreType.DMA((3, 8)),
                pltpu.SemaphoreType.DMA((3, 8)),
            ],
            compiler_params=pltpu.CompilerParams(collective_id=0, has_side_effects=True),
        )(tiles, metric_diag.transpose(1, 0, 2), metric_cross, point_mass)
        return result.reshape(rows, cols, nfield, lanes).transpose(2, 0, 1, 3)

    return jax.shard_map(
        shards,
        mesh=mesh,
        in_specs=(
            P(None, "face", "col", None),
            P(None, "face", "col"),
            P("face", "col"),
            P("face", "col"),
        ),
        out_specs=P(None, "face", "col", None),
        check_vma=False,
    )
```
